256 devices in a mesh: rep: 8 (over x_lo, y), ep: 32 (over x_hi, z, core).
Axes of the slice: x: 4 (x_hi: 2, x_lo: 2; x = x_hi * 2 + x_lo), y: 4, z: 8, core: 2. Of those that a mesh axis runs over, the one named last changes fastest.
Arguments:
- hidden: bfloat16 [4, 8192, 2, 2048], P(None, ('rep', 'ep')), may hold values from -6 to 6
- out_grad: bfloat16 [4, 8192, 7168], P(None, ('rep', 'ep')), may hold values from -0.5 to 0.5
- route_weight: float32 [4, 8192, 2], P(None, ('rep', 'ep')), may hold values from 0.05 to 1
- expert_ids: int32 [4, 8192, 2], P(None, ('rep', 'ep')), may hold values from 0 to 31, as said below
Outputs:
- grad_down: bfloat16 [32, 2048, 7168], P('ep', None, 'rep')
- expert_load: float32 [32], replicated
The draws below stay inside these ranges and needn't reach their ends.
Inputs may be any that keep to these rules, and one draw needn't show every extreme that they name: `expert_ids`: in each micro-batch the 32 tokens of one device (aligned blocks of 32 tokens) name no expert in more than 4 pairs, and some expert is named in exactly 4; the 2 experts of a token differ.
All inputs are finite; a program needn't handle non-finite values.
Results may differ from the reference program's by a relative error of at most 0.0049.
Values may be sent and summed in bfloat16 or wider, within the bound.
A program may use at most 192 MiB of HBM per device.

```python
import math
import jax
import jax.numpy as jnp
from jax import lax

D = 7168
FF = 2048
TOK_DEV = 32
MICRO = 4
TOPK = 2
SPECIALIST_COUNT = 32
TOKENS = 8192
CAP = 4
N_REP = 8
N_EP = 32


def dispatched_specialist_group(group_seed_value, position_affinity_boost, position_specialist_pick):
    slot_total = SPECIALIST_COUNT * CAP
    noise_key, forced_key, order_key, turn_key = jax.random.split(group_seed_value, 4)
    gaussian_perturbation = jax.random.randint(noise_key, (slot_total,), 0, 65536, dtype=jnp.int32)
    mandated_specialists = jax.random.randint(forced_key, (), 0, SPECIALIST_COUNT, dtype=jnp.int32)
    plain_affinity = jnp.where(position_specialist_pick == mandated_specialists, jnp.int32(262144), position_affinity_boost + gaussian_perturbation)
    score = plain_affinity * slot_total + jnp.arange(slot_total, dtype=jnp.int32)
    chosen = lax.top_k(score, TOK_DEV * TOPK)[1].astype(jnp.int32)
    ordered = jnp.sort(chosen)
    experts = (ordered // CAP).reshape(TOPK, TOK_DEV).T
    token_order = jax.random.permutation(order_key, TOK_DEV).astype(jnp.int32)
    experts = experts[token_order]
    turn = jax.random.randint(turn_key, (TOK_DEV,), 0, TOPK, dtype=jnp.int32)
    column = (jnp.arange(TOPK, dtype=jnp.int32)[None, :] + turn[:, None]) % TOPK
    return jnp.take_along_axis(experts, column, axis=1).astype(jnp.int32)


def draw_expert_ids(key, part):
    rank_key, group_seed_value = jax.random.split(jax.random.fold_in(key, 7101))
    specialist_ordering = jax.random.permutation(rank_key, SPECIALIST_COUNT).astype(jnp.int32)
    affinity_boost = specialist_ordering * 49152 // SPECIALIST_COUNT
    position_specialist_pick = jnp.arange(SPECIALIST_COUNT * CAP, dtype=jnp.int32) // CAP
    position_affinity_boost = affinity_boost[position_specialist_pick]
    block_total = MICRO * (TOKENS // TOK_DEV)
    group_seed_values = jax.random.split(group_seed_value, block_total)
    dispatched_specialists = jax.vmap(lambda lone_specialist: dispatched_specialist_group(lone_specialist, position_affinity_boost, position_specialist_pick))(group_seed_values)
    return dispatched_specialists.reshape(MICRO, TOKENS, TOPK).astype(jnp.int32)


def strengthened(drawn, own_key, source, target, parts, factor):
    owner, partner = [(jnp.arange(drawn.shape[position]) // (drawn.shape[position] // parts)).reshape([-1 if axis == position else 1 for axis in range(drawn.ndim)]) for position in (source, target)]
    chosen = jax.random.permutation(own_key, parts)[partner]
    strong = (owner == chosen) | (owner == (partner + parts // 2) % parts)
    return jnp.where(strong, factor * drawn, drawn)


def level_of(own_key, shape, cuts, least, top_value):
    def one(dim, blocks):
        steps = jax.random.uniform(jax.random.fold_in(jax.random.fold_in(own_key, 6), dim), (blocks,), jnp.float32, least / len(cuts), top_value / len(cuts))
        return jnp.repeat(jnp.exp(steps), shape[dim] // blocks).reshape((-1,) + (1,) * (len(shape) - dim - 1))

    gain = one(*cuts[0])
    for cut in cuts[1:]:
        gain = gain * one(*cut)
    return gain


def gaussian(key, shape, width, limit, pieces=(), held_as=jnp.bfloat16):
    array = jax.random.normal(key, shape, jnp.float32) * width
    if len(pieces) > 0:
        array = level_of(key, shape, pieces, -0.22, 0.18) * array
    return jnp.clip(array, min=-limit, max=limit).astype(held_as)


def bell_draw_with(own_key, shape, width, limit, cuts, heavy, kind=jnp.bfloat16):
    result = width * jax.random.normal(own_key, shape, jnp.float32)
    if cuts:
        result = result * level_of(own_key, shape, cuts, -0.22, 0.18)
    return jnp.clip(strengthened(result, jax.random.fold_in(own_key, 3), *heavy), -limit, limit).astype(kind)


def setup_inputs(seed: int = 0) -> dict:
    arg_keys = jax.random.split(jax.random.key(seed), 5)
    return {
        "hidden": gaussian(arg_keys[0], (MICRO, TOKENS, TOPK, FF), 1.0, 6.0, ((1, 256),)),
        "out_grad": bell_draw_with(arg_keys[1], (MICRO, TOKENS, D), ((MICRO * TOK_DEV * TOPK * N_REP) ** -0.5), 0.5, ((1, 256),), (1, 2, 256, 6.0)),
        "route_weight": jnp.clip(jnp.exp(math.log(1.0) - 2.9957323 * jax.random.uniform(arg_keys[2], (MICRO, TOKENS, TOPK), jnp.float32) ** level_of(arg_keys[2], (MICRO, TOKENS, TOPK), ((1, 256),), -0.2, 0.2)), 0.05, 1.0),
        "expert_ids": draw_expert_ids(jax.random.fold_in(arg_keys[4], 71), 0),
    }


def reference(hidden, out_grad, route_weight, expert_ids):
    scaled = (route_weight[:, :, :, None] * out_grad[:, :, None, :].astype(jnp.float32)).astype(jnp.bfloat16)
    pair_hidden = hidden.reshape(-1, FF)
    pair_grad = scaled.reshape(-1, D)
    flat_routes = expert_ids.reshape(-1)
    largest = MICRO * N_REP * N_EP * CAP

    def one_expert(expert):
        chosen = flat_routes == expert
        picked = jnp.nonzero(chosen, size=largest, fill_value=0)[0]
        usable = jnp.arange(largest) < jnp.sum(chosen.astype(jnp.int32))
        selected = jnp.where(usable[:, None], pair_hidden[picked], jnp.zeros((), hidden.dtype))
        product = lax.dot_general(selected, pair_grad[picked], (((0,), (0,)), ((), ())), preferred_element_type=jnp.float32)
        return product.astype(jnp.bfloat16)

    grad_down = lax.map(one_expert, jnp.arange(SPECIALIST_COUNT, dtype=jnp.int32))
    tallies = jnp.sum((flat_routes[:, None] == jnp.arange(SPECIALIST_COUNT, dtype=jnp.int32)[None, :]).astype(jnp.float32), axis=0)
    expert_load = tallies * (SPECIALIST_COUNT / (MICRO * TOKENS * TOPK))
    return grad_down, expert_load
```

```python
import functools

import jax
import jax.numpy as jnp
from jax import lax
from jax.experimental import pallas as pl
from jax.experimental.pallas import tpu as pltpu
from jax.sharding import Mesh
from jax.sharding import PartitionSpec as P

REP_EP = ("rep_0", "rep_1", "ep_0", "ep_1", "ep_2")
EP = ("ep_0", "ep_1", "ep_2")
REP = ("rep_0", "rep_1")
MESH = pl.DeviceIdType.MESH
NX, NY, NZ, NC = 4, 4, 8, 2
NE = NZ * NC
NQ = NX * NY
ZC = [(1, 0), (7, 0), (1, 1), (7, 1), (2, 0), (6, 0), (2, 1), (6, 1), (3, 0), (5, 0), (3, 1), (5, 1), (4, 0), (4, 1), (0, 1)]
GROUP_DY = [0, 1, 3, 2]


def kernel(hid_ref, slot_ref, meta_ref, og_ref, out_ref, load_ref,
           graw, meta, gsend, gall, hp, hz, hzt, ht, acc, cnt, cnt_all,
           s_send, s_meta, s_graw, s_gz, s_hz, s_hx, s_hy, s_cnt, s_local):
    cap = hp.shape[2]
    ff = hzt.shape[1]
    cols = graw.shape[3]
    rows = NE * cap
    toks = graw.shape[1] * graw.shape[2]
    xlo, y = lax.axis_index("rep_0"), lax.axis_index("rep_1")
    xhi, z, core = lax.axis_index("ep_0"), lax.axis_index("ep_1"), lax.axis_index("ep_2")
    x = xhi * 2 + xlo
    me = z * NC + core

    def plane(dx, dy):
        x2, y2 = lax.rem(x + dx, NX), lax.rem(y + dy, NY)
        return x2, y2, {"rep_0": lax.rem(x2, 2), "rep_1": y2, "ep_0": x2 // 2}

    def zc(dz, dc):
        z2, c2 = lax.rem(z + dz, NZ), lax.rem(core + dc, NC)
        return z2 * NC + c2, {"ep_1": z2, "ep_2": c2}

    def send(src, dst, send_sem, recv_sem, dev):
        pltpu.make_async_remote_copy(
            src_ref=src, dst_ref=dst, send_sem=send_sem, recv_sem=recv_sem, device_id=dev, device_id_type=MESH
        ).start()

    def wait(ref, sem):
        pltpu.make_async_copy(ref, ref, sem).wait()

    barrier = pltpu.get_barrier_semaphore()
    for dy in range(NY):
        for dx in range(NX):
            if dx or dy:
                pl.semaphore_signal(barrier, inc=1, device_id=plane(dx, dy)[2], device_id_type=MESH)
    for dz, dc in ZC:
        pl.semaphore_signal(barrier, inc=1, device_id=zc(dz, dc)[1], device_id_type=MESH)
    pl.semaphore_wait(barrier, NQ - 1 + NE - 1)

    for group in range(NY):
        dy = (NY - GROUP_DY[group]) % NY
        for dx in (0, 1, 3, 2):
            if not (dx or dy):
                continue
            _, y2, dev = plane(dx, dy)
            send(meta_ref, meta.at[group * NX + x], s_send.at[0], s_meta, dev)
        for dx in (0, 1, 3, 2):
            if not (dx or dy):
                continue
            x2, y2, dev = plane(dx, dy)
            at = pl.multiple_of((lax.rem(x2, 2) * NY + y2) * cols, 128)
            send(og_ref.at[:, :, pl.ds(at, cols)], graw.at[group * NX + x], s_send.at[1], s_graw.at[group], dev)
    mine = pl.multiple_of((xlo * NY + y) * cols, 128)
    own_g = pltpu.make_async_copy(og_ref.at[:, :, pl.ds(mine, cols)], graw.at[x], s_local.at[0])
    own_g.start()
    own_m = pltpu.make_async_copy(meta_ref, meta.at[x], s_local.at[1])
    own_m.start()

    half = NE * cap
    pairs = hid_ref.shape[0]
    for i in range(2):
        sel = jnp.where(
            lax.broadcasted_iota(jnp.int32, (half, pairs), 0) + i * half == slot_ref[...], 1.0, 0.0
        ).astype(jnp.bfloat16)
        for c in range(0, ff, 512):
            packed = jnp.dot(sel, hid_ref[:, c:c + 512], preferred_element_type=jnp.float32)
            hp[i, :, :, c:c + 512] = packed.astype(jnp.bfloat16).reshape(NE, cap, 512)
    own_m.wait()
    own_g.wait()
    wait(meta.at[pl.ds(0, NQ - 1)], s_meta)
    total = meta[0]
    for q in range(1, NQ):
        total = total + meta[q]
    cnt[...] = total
    for dz, dc in ZC:
        e, dev = zc(dz, dc)
        send(hp.at[:, e], hz.at[:, me], s_send.at[2], s_hz, dev)
    own_h = pltpu.make_async_copy(hp.at[:, me], hz.at[:, me], s_local.at[2])
    own_h.start()

    def pack_and_send(group):
        if group:
            wait(graw.at[pl.ds(group * NX, NX)], s_graw.at[group])
        else:
            wait(graw.at[pl.ds(0, NX - 1)], s_graw.at[0])
        slot_of_row = (lax.broadcasted_iota(jnp.int32, (rows, toks), 0) + xhi * rows).astype(jnp.float32)
        for xs in range(NX):
            q = group * NX + xs
            info = meta[q]
            first = slot_of_row == info[0:1, :]
            second = slot_of_row == info[1:2, :]
            weights = jnp.where(first, info[2:3, :], jnp.where(second, info[3:4, :], 0.0))
            weight = jnp.sum(weights, axis=1, keepdims=True)
            sel = jnp.where(first | second, 1.0, 0.0).astype(jnp.bfloat16)
            raw = graw[q].reshape(toks, cols)
            packed = jnp.dot(sel, raw, preferred_element_type=jnp.float32) * weight
            gsend[q] = packed.astype(jnp.bfloat16).reshape(NE, cap, cols)
        part = pl.ds(group * NX, NX)
        for dz, dc in ZC:
            e, dev = zc(dz, dc)
            send(gsend.at[part, e], gall.at[part, me], s_send.at[3], s_gz.at[group], dev)
        own = pltpu.make_async_copy(gsend.at[part, me], gall.at[part, me], s_local.at[3 + group])
        own.start()
        return own

    owns = [pack_and_send(0), pack_and_send(1), pack_and_send(2)]

    own_h.wait()
    wait(hz.at[:, pl.ds(0, NE - 1)], s_hz)
    eye = jnp.where(
        lax.broadcasted_iota(jnp.int32, (256, 256), 0) == lax.broadcasted_iota(jnp.int32, (256, 256), 1), 1.0, 0.0
    ).astype(jnp.bfloat16)
    for i in range(2):
        for c in range(0, ff, 256):
            block = hz[i, :, :, c:c + 256].reshape(rows, 256)
            turned = lax.dot_general(eye, block, (((1,), (1,)), ((), ())), preferred_element_type=jnp.float32)
            hzt[i, c:c + 256, :] = turned.astype(jnp.bfloat16)
    for dz, dc in ZC:
        e, dev = zc(dz, dc)
        send(cnt, cnt_all.at[me], s_send.at[4], s_cnt, dev)
    for dx in (1, 3, 2):
        x2, _, dev = plane(dx, 0)
        send(hzt.at[x2 // 2], ht.at[x], s_send.at[5], s_hx.at[x], dev)
    own_t = pltpu.make_async_copy(hzt.at[xhi], ht.at[x], s_local.at[7])
    own_t.start()

    owns.append(pack_and_send(3))

    _, _, up = plane(0, 1)
    _, _, down = plane(0, 3)
    hf = ff // 2

    def to_row(xs):
        send(ht.at[xs], ht.at[2 * NX + xs], s_send.at[6], s_hy.at[0, xs], up)
        send(ht.at[xs], ht.at[NX + xs], s_send.at[6], s_hy.at[1, xs], down)

    own_t.wait()
    to_row(x)
    for dx in (1, 3, 2):
        xs = lax.rem(x + dx, NX)
        wait(ht.at[xs], s_hx.at[xs])
        to_row(xs)
    for dx in (0, 1, 3, 2):
        xs = lax.rem(x + dx, NX)
        wait(ht.at[2 * NX + xs], s_hy.at[0, xs])
        send(ht.at[2 * NX + xs, pl.ds(0, hf)], ht.at[3 * NX + xs, pl.ds(0, hf)], s_send.at[7], s_hy.at[2, xs], up)
        wait(ht.at[NX + xs], s_hy.at[1, xs])
        send(ht.at[NX + xs, pl.ds(hf, hf)], ht.at[3 * NX + xs, pl.ds(hf, hf)], s_send.at[7], s_hy.at[3, xs], down)

    tile = 512
    for group in range(NY):
        owns[group].wait()
        wait(gall.at[pl.ds(group * NX, NX), pl.ds(0, NE - 1)], s_gz.at[group])
        if group == NY - 1:
            for xs in range(NX):
                wait(ht.at[3 * NX + xs, pl.ds(0, hf)], s_hy.at[2, xs])
                wait(ht.at[3 * NX + xs, pl.ds(hf, hf)], s_hy.at[3, xs])

        @pl.loop(0, ff // tile)
        def _(m):
            at = pl.ds(pl.multiple_of(m * tile, tile), tile)
            part = None
            for xs in range(NX):
                q = group * NX + xs
                term = jnp.dot(ht[q, at, :], gall[q].reshape(rows, cols), preferred_element_type=jnp.float32)
                part = term if part is None else part + term
            if group == 0:
                acc[at, :] = part
            elif group < NY - 1:
                acc[at, :] += part
            else:
                out_ref[0, at, :] = (acc[at, :] + part).astype(out_ref.dtype)

    wait(cnt_all.at[pl.ds(0, NE - 1)], s_cnt)
    cnt_all[me] = cnt[...]
    loads = cnt_all[0]
    for e in range(1, NE):
        loads = loads + cnt_all[e]
    load_ref[...] = loads

    wait(meta.at[pl.ds(0, NQ - 1)], s_send.at[0])
    wait(graw.at[pl.ds(0, NQ - 1)], s_send.at[1])
    wait(hz.at[:, pl.ds(0, NE - 1)], s_send.at[2])
    wait(gall.at[:, pl.ds(0, NE - 1)], s_send.at[3])
    wait(cnt_all.at[pl.ds(0, NE - 1)], s_send.at[4])
    wait(ht.at[pl.ds(0, NX - 1)], s_send.at[5])
    wait(ht.at[pl.ds(0, 2 * NX)], s_send.at[6])
    wait(ht.at[pl.ds(0, NX)], s_send.at[7])


def body(hidden, out_grad, route_weight, expert_ids):
    micro, tokens, picks, ff = hidden.shape
    width = out_grad.shape[2]
    experts = lax.axis_size(EP)
    replicas = lax.axis_size(REP)
    cols = width // replicas
    limit = 2 * tokens * picks // experts
    cap = micro * limit
    toks = micro * tokens
    ids = expert_ids.reshape(micro, tokens * picks)
    order = jnp.arange(tokens * picks, dtype=jnp.int32)
    earlier = (ids[:, :, None] == ids[:, None, :]) & (order[None, None, :] < order[None, :, None])
    position = jnp.sum(earlier.astype(jnp.int32), axis=2)
    slot = ids * cap + jnp.arange(micro, dtype=jnp.int32)[:, None] * limit + position
    by_token = slot.reshape(toks, picks).T.astype(jnp.float32)
    weights = route_weight.reshape(toks, picks).T
    tally = jnp.sum(
        (expert_ids.reshape(toks * picks)[None, :] == jnp.arange(toks, dtype=jnp.int32)[:, None]).astype(jnp.float32),
        axis=1,
    )
    meta = jnp.concatenate([by_token, weights, tally[None, :], jnp.zeros((3, toks), jnp.float32)], axis=0)
    vmem = pl.BlockSpec(memory_space=pltpu.VMEM)
    bf16 = jnp.bfloat16
    dma = pltpu.SemaphoreType.DMA
    grad, load = pl.pallas_call(
        kernel,
        out_shape=(
            jax.ShapeDtypeStruct((1, ff, cols), bf16),
            jax.ShapeDtypeStruct((8, toks), jnp.float32),
        ),
        in_specs=[vmem, vmem, vmem, pl.BlockSpec(memory_space=pl.ANY)],
        out_specs=(vmem, vmem),
        scratch_shapes=[
            pltpu.VMEM((NQ, micro, tokens, cols), bf16),
            pltpu.VMEM((NQ, 8, toks), jnp.float32),
            pltpu.VMEM((NQ, NE, cap, cols), bf16),
            pltpu.VMEM((NQ, NE, cap, cols), bf16),
            pltpu.VMEM((2, NE, cap, ff), bf16),
            pltpu.VMEM((2, NE, cap, ff), bf16),
            pltpu.VMEM((2, ff, NE * cap), bf16),
            pltpu.VMEM((NQ, ff, NE * cap), bf16),
            pltpu.VMEM((ff, cols), jnp.float32),
            pltpu.VMEM((8, toks), jnp.float32),
            pltpu.VMEM((NE, 8, toks), jnp.float32),
            dma((8,)),
            dma,
            dma((NY,)),
            dma((NY,)),
            dma,
            dma((NX,)),
            dma((4, NX)),
            dma,
            dma((8,)),
        ],
        compiler_params=pltpu.CompilerParams(
            collective_id=0, has_side_effects=True, vmem_limit_bytes=66 * 1024 * 1024 - 4 * 1024 * 1024
        ),
    )(hidden.reshape(toks * picks, ff), slot.reshape(1, toks * picks), meta, out_grad)
    expert_load = load[4, :experts] / float(micro * tokens * replicas * picks)
    return grad, expert_load


def solution(mesh):
    finer = Mesh(mesh.devices.reshape(2, 4, 2, 8, 2), REP_EP)
    placed = (
        P(None, REP_EP, None, None),
        P(None, REP_EP, None),
        P(None, REP_EP, None),
        P(None, REP_EP, None),
    )
    return jax.shard_map(
        body, mesh=finer, in_specs=placed, out_specs=(P(EP, None, REP), P()), check_vma=False
    )
```

```python
import functools

import jax
import jax.numpy as jnp
from jax import lax
from jax.experimental import pallas as pl
from jax.experimental.pallas import tpu as pltpu
from jax.sharding import Mesh
from jax.sharding import PartitionSpec as P

REP_EP = ("rep_0", "rep_1", "ep_0", "ep_1", "ep_2")
EP = ("ep_0", "ep_1", "ep_2")
REP = ("rep_0", "rep_1")
MESH = pl.DeviceIdType.MESH
NX, NY, NZ, NC = 4, 4, 8, 2
NE = NZ * NC
NQ = NX * NY
ZC = [(1, 0), (7, 0), (1, 1), (7, 1), (2, 0), (6, 0), (2, 1), (6, 1), (3, 0), (5, 0), (3, 1), (5, 1), (4, 0), (4, 1), (0, 1)]
GROUP_DY = [0, 1, 3, 2]


def kernel(hid_ref, slot_ref, meta_ref, og_ref, out_ref, load_ref,
           graw, meta, gsend, gall, hp, hz, hzt, ht, acc, cnt, cnt_all,
           s_send, s_meta, s_graw, s_gz, s_hz, s_hx, s_hy, s_cnt, s_local):
    cap = hp.shape[2]
    ff = hzt.shape[1]
    cols = graw.shape[3]
    rows = NE * cap
    toks = graw.shape[1] * graw.shape[2]
    xlo, y = lax.axis_index("rep_0"), lax.axis_index("rep_1")
    xhi, z, core = lax.axis_index("ep_0"), lax.axis_index("ep_1"), lax.axis_index("ep_2")
    x = xhi * 2 + xlo
    me = z * NC + core

    def plane(dx, dy):
        x2, y2 = lax.rem(x + dx, NX), lax.rem(y + dy, NY)
        return x2, y2, {"rep_0": lax.rem(x2, 2), "rep_1": y2, "ep_0": x2 // 2}

    def zc(dz, dc):
        z2, c2 = lax.rem(z + dz, NZ), lax.rem(core + dc, NC)
        return z2 * NC + c2, {"ep_1": z2, "ep_2": c2}

    def send(src, dst, send_sem, recv_sem, dev):
        pltpu.make_async_remote_copy(
            src_ref=src, dst_ref=dst, send_sem=send_sem, recv_sem=recv_sem, device_id=dev, device_id_type=MESH
        ).start()

    def wait(ref, sem):
        pltpu.make_async_copy(ref, ref, sem).wait()

    barrier = pltpu.get_barrier_semaphore()
    for dy in range(NY):
        for dx in range(NX):
            if dx or dy:
                pl.semaphore_signal(barrier, inc=1, device_id=plane(dx, dy)[2], device_id_type=MESH)
    for dz, dc in ZC:
        pl.semaphore_signal(barrier, inc=1, device_id=zc(dz, dc)[1], device_id_type=MESH)
    pl.semaphore_wait(barrier, NQ - 1 + NE - 1)

    for group in range(NY):
        dy = (NY - GROUP_DY[group]) % NY
        for dx in (0, 1, 3, 2):
            if dx or dy:
                send(meta_ref, meta.at[group * NX + x], s_send.at[0], s_meta, plane(dx, dy)[2])
    for group in range(NY):
        dy = (NY - GROUP_DY[group]) % NY
        for dx in (0, 1, 3, 2):
            if not (dx or dy):
                continue
            x2, y2, dev = plane(dx, dy)
            at = pl.multiple_of((lax.rem(x2, 2) * NY + y2) * cols, 128)
            send(og_ref.at[:, :, pl.ds(at, cols)], graw.at[group * NX + x], s_send.at[1], s_graw.at[group], dev)
    mine = pl.multiple_of((xlo * NY + y) * cols, 128)
    own_g = pltpu.make_async_copy(og_ref.at[:, :, pl.ds(mine, cols)], graw.at[x], s_local.at[0])
    own_g.start()
    own_m = pltpu.make_async_copy(meta_ref, meta.at[x], s_local.at[1])
    own_m.start()

    half = NE * cap
    pairs = hid_ref.shape[0]
    for i in range(2):
        sel = jnp.where(
            lax.broadcasted_iota(jnp.int32, (half, pairs), 0) + i * half == slot_ref[...], 1.0, 0.0
        ).astype(jnp.bfloat16)
        for c in range(0, ff, 512):
            packed = jnp.dot(sel, hid_ref[:, c:c + 512], preferred_element_type=jnp.float32)
            hp[i, :, :, c:c + 512] = packed.astype(jnp.bfloat16).reshape(NE, cap, 512)
    own_m.wait()
    own_g.wait()
    for dz, dc in ZC:
        e, dev = zc(dz, dc)
        send(hp.at[:, e], hz.at[:, me], s_send.at[2], s_hz, dev)
    own_h = pltpu.make_async_copy(hp.at[:, me], hz.at[:, me], s_local.at[2])
    own_h.start()
    wait(meta.at[pl.ds(0, NQ - 1)], s_meta)
    total = meta[0]
    for q in range(1, NQ):
        total = total + meta[q]
    cnt[...] = total

    def pack_and_send(group):
        if group:
            wait(graw.at[pl.ds(group * NX, NX)], s_graw.at[group])
        else:
            wait(graw.at[pl.ds(0, NX - 1)], s_graw.at[0])
        slot_of_row = (lax.broadcasted_iota(jnp.int32, (rows, toks), 0) + xhi * rows).astype(jnp.float32)
        for xs in range(NX):
            q = group * NX + xs
            info = meta[q]
            first = slot_of_row == info[0:1, :]
            second = slot_of_row == info[1:2, :]
            weights = jnp.where(first, info[2:3, :], jnp.where(second, info[3:4, :], 0.0))
            weight = jnp.sum(weights, axis=1, keepdims=True)
            sel = jnp.where(first | second, 1.0, 0.0).astype(jnp.bfloat16)
            raw = graw[q].reshape(toks, cols)
            packed = jnp.dot(sel, raw, preferred_element_type=jnp.float32) * weight
            gsend[q] = packed.astype(jnp.bfloat16).reshape(NE, cap, cols)
        part = pl.ds(group * NX, NX)
        for dz, dc in ZC:
            e, dev = zc(dz, dc)
            send(gsend.at[part, e], gall.at[part, me], s_send.at[3], s_gz.at[group], dev)
        own = pltpu.make_async_copy(gsend.at[part, me], gall.at[part, me], s_local.at[3 + group])
        own.start()
        return own

    owns = [pack_and_send(0), pack_and_send(1), pack_and_send(2)]

    own_h.wait()
    wait(hz.at[:, pl.ds(0, NE - 1)], s_hz)
    eye = jnp.where(
        lax.broadcasted_iota(jnp.int32, (256, 256), 0) == lax.broadcasted_iota(jnp.int32, (256, 256), 1), 1.0, 0.0
    ).astype(jnp.bfloat16)
    for i in range(2):
        for c in range(0, ff, 256):
            block = hz[i, :, :, c:c + 256].reshape(rows, 256)
            turned = lax.dot_general(eye, block, (((1,), (1,)), ((), ())), preferred_element_type=jnp.float32)
            hzt[i, c:c + 256, :] = turned.astype(jnp.bfloat16)
    for dz, dc in ZC:
        e, dev = zc(dz, dc)
        send(cnt, cnt_all.at[me], s_send.at[4], s_cnt, dev)
    for dx in (1, 3, 2):
        x2, _, dev = plane(dx, 0)
        send(hzt.at[x2 // 2], ht.at[x], s_send.at[5], s_hx.at[x], dev)
    own_t = pltpu.make_async_copy(hzt.at[xhi], ht.at[x], s_local.at[7])
    own_t.start()

    owns.append(pack_and_send(3))

    _, _, up = plane(0, 1)
    _, _, down = plane(0, 3)
    hf = ff // 2

    def to_row(xs):
        send(ht.at[xs], ht.at[2 * NX + xs], s_send.at[6], s_hy.at[0, xs], up)
        send(ht.at[xs], ht.at[NX + xs], s_send.at[6], s_hy.at[1, xs], down)

    own_t.wait()
    to_row(x)
    for dx in (1, 3, 2):
        xs = lax.rem(x + dx, NX)
        wait(ht.at[xs], s_hx.at[xs])
        to_row(xs)
    for dx in (0, 1, 3, 2):
        xs = lax.rem(x + dx, NX)
        wait(ht.at[2 * NX + xs], s_hy.at[0, xs])
        send(ht.at[2 * NX + xs, pl.ds(0, hf)], ht.at[3 * NX + xs, pl.ds(0, hf)], s_send.at[7], s_hy.at[2, xs], up)
        wait(ht.at[NX + xs], s_hy.at[1, xs])
        send(ht.at[NX + xs, pl.ds(hf, hf)], ht.at[3 * NX + xs, pl.ds(hf, hf)], s_send.at[7], s_hy.at[3, xs], down)

    tile = 512
    for group in range(NY):
        owns[group].wait()
        wait(gall.at[pl.ds(group * NX, NX), pl.ds(0, NE - 1)], s_gz.at[group])
        if group == NY - 1:
            for xs in range(NX):
                wait(ht.at[3 * NX + xs, pl.ds(0, hf)], s_hy.at[2, xs])
                wait(ht.at[3 * NX + xs, pl.ds(hf, hf)], s_hy.at[3, xs])

        @pl.loop(0, ff // tile)
        def _(m):
            at = pl.ds(pl.multiple_of(m * tile, tile), tile)
            part = None
            for xs in range(NX):
                q = group * NX + xs
                term = jnp.dot(ht[q, at, :], gall[q].reshape(rows, cols), preferred_element_type=jnp.float32)
                part = term if part is None else part + term
            if group == 0:
                acc[at, :] = part
            elif group < NY - 1:
                acc[at, :] += part
            else:
                out_ref[0, at, :] = (acc[at, :] + part).astype(out_ref.dtype)

    wait(cnt_all.at[pl.ds(0, NE - 1)], s_cnt)
    cnt_all[me] = cnt[...]
    loads = cnt_all[0]
    for e in range(1, NE):
        loads = loads + cnt_all[e]
    load_ref[...] = loads

    wait(meta.at[pl.ds(0, NQ - 1)], s_send.at[0])
    wait(graw.at[pl.ds(0, NQ - 1)], s_send.at[1])
    wait(hz.at[:, pl.ds(0, NE - 1)], s_send.at[2])
    wait(gall.at[:, pl.ds(0, NE - 1)], s_send.at[3])
    wait(cnt_all.at[pl.ds(0, NE - 1)], s_send.at[4])
    wait(ht.at[pl.ds(0, NX - 1)], s_send.at[5])
    wait(ht.at[pl.ds(0, 2 * NX)], s_send.at[6])
    wait(ht.at[pl.ds(0, NX)], s_send.at[7])


def body(hidden, out_grad, route_weight, expert_ids):
    micro, tokens, picks, ff = hidden.shape
    width = out_grad.shape[2]
    experts = lax.axis_size(EP)
    replicas = lax.axis_size(REP)
    cols = width // replicas
    limit = 2 * tokens * picks // experts
    cap = micro * limit
    toks = micro * tokens
    ids = expert_ids.reshape(micro, tokens * picks)
    order = jnp.arange(tokens * picks, dtype=jnp.int32)
    earlier = (ids[:, :, None] == ids[:, None, :]) & (order[None, None, :] < order[None, :, None])
    position = jnp.sum(earlier.astype(jnp.int32), axis=2)
    slot = ids * cap + jnp.arange(micro, dtype=jnp.int32)[:, None] * limit + position
    by_token = slot.reshape(toks, picks).T.astype(jnp.float32)
    weights = route_weight.reshape(toks, picks).T
    tally = jnp.sum(
        (expert_ids.reshape(toks * picks)[None, :] == jnp.arange(toks, dtype=jnp.int32)[:, None]).astype(jnp.float32),
        axis=1,
    )
    meta = jnp.concatenate([by_token, weights, tally[None, :], jnp.zeros((3, toks), jnp.float32)], axis=0)
    vmem = pl.BlockSpec(memory_space=pltpu.VMEM)
    bf16 = jnp.bfloat16
    dma = pltpu.SemaphoreType.DMA
    grad, load = pl.pallas_call(
        kernel,
        out_shape=(
            jax.ShapeDtypeStruct((1, ff, cols), bf16),
            jax.ShapeDtypeStruct((8, toks), jnp.float32),
        ),
        in_specs=[vmem, vmem, vmem, pl.BlockSpec(memory_space=pl.ANY)],
        out_specs=(vmem, vmem),
        scratch_shapes=[
            pltpu.VMEM((NQ, micro, tokens, cols), bf16),
            pltpu.VMEM((NQ, 8, toks), jnp.float32),
            pltpu.VMEM((NQ, NE, cap, cols), bf16),
            pltpu.VMEM((NQ, NE, cap, cols), bf16),
            pltpu.VMEM((2, NE, cap, ff), bf16),
            pltpu.VMEM((2, NE, cap, ff), bf16),
            pltpu.VMEM((2, ff, NE * cap), bf16),
            pltpu.VMEM((NQ, ff, NE * cap), bf16),
            pltpu.VMEM((ff, cols), jnp.float32),
            pltpu.VMEM((8, toks), jnp.float32),
            pltpu.VMEM((NE, 8, toks), jnp.float32),
            dma((8,)),
            dma,
            dma((NY,)),
            dma((NY,)),
            dma,
            dma((NX,)),
            dma((4, NX)),
            dma,
            dma((8,)),
        ],
        compiler_params=pltpu.CompilerParams(
            collective_id=0, has_side_effects=True, vmem_limit_bytes=66 * 1024 * 1024 - 4 * 1024 * 1024
        ),
    )(hidden.reshape(toks * picks, ff), slot.reshape(1, toks * picks), meta, out_grad)
    expert_load = load[4, :experts] / float(micro * tokens * replicas * picks)
    return grad, expert_load


def solution(mesh):
    finer = Mesh(mesh.devices.reshape(2, 4, 2, 8, 2), REP_EP)
    placed = (
        P(None, REP_EP, None, None),
        P(None, REP_EP, None),
        P(None, REP_EP, None),
        P(None, REP_EP, None),
    )
    return jax.shard_map(
        body, mesh=finer, in_specs=placed, out_specs=(P(EP, None, REP), P()), check_vma=False
    )
```

```python
import functools

import jax
import jax.numpy as jnp
from jax import lax
from jax.experimental import pallas as pl
from jax.experimental.pallas import tpu as pltpu
from jax.sharding import Mesh
from jax.sharding import PartitionSpec as P

REP_EP = ("rep_0", "rep_1", "ep_0", "ep_1", "ep_2")
EP = ("ep_0", "ep_1", "ep_2")
REP = ("rep_0", "rep_1")
MESH = pl.DeviceIdType.MESH
NX, NY, NZ, NC = 4, 4, 8, 2
NE = NZ * NC
NQ = NX * NY
NEAR = 5
CHUNKS = 4
ZC = [(1, 0), (7, 0), (1, 1), (7, 1), (2, 0), (6, 0), (2, 1), (6, 1), (3, 0), (5, 0), (3, 1), (5, 1), (4, 0), (4, 1), (0, 1)]
GROUP_DY = [0, 1, 3, 2]
ORDER = [
    ("hid", 0), ("routes", 0), ("raw", 0), ("hid", 1), ("turn", 0), ("raw", 1), ("far", 0), ("row", 0), ("hid", 2),
    ("raw", 2), ("turn", 1), ("far", 1), ("pack", 0), ("row", 1), ("relay", 0), ("hid", 3), ("raw", 3), ("turn", 2),
    ("far", 2), ("pack", 1), ("row", 2), ("relay", 1), ("turn", 3), ("far", 3), ("row", 3), ("pack", 2), ("relay", 2),
    ("pack", 3), ("relay", 3),
    ("mul", 0, 0, 4), ("mul", 1, 0, 4), ("mul", 2, 0, 4), ("mul", 3, 0, 4),
]


def kernel(hid_ref, slot_ref, meta_ref, og_ref, out_ref, load_ref,
           graw, meta, gnear, gfar, gall, hp, hz, hzt, ht, acc, cnt, cnt_all, cnt_x,
           s_send, s_meta, s_first, s_raw, s_gz, s_hz, s_hx, s_hy, s_cnt):
    cap, step = hp.shape[3], hp.shape[4]
    cols = graw.shape[5]
    toks = graw.shape[3] * graw.shape[4]
    pairs = hid_ref.shape[0]
    xlo, y = lax.axis_index("rep_0"), lax.axis_index("rep_1")
    xhi, z, core = lax.axis_index("ep_0"), lax.axis_index("ep_1"), lax.axis_index("ep_2")
    x = xhi * 2 + xlo

    def in_plane(dxl, dy):
        x2, y2 = lax.rem(xlo + dxl, 2), lax.rem(y + dy, NY)
        return x2, y2, {"rep_0": x2, "rep_1": y2}

    def along_x(dx):
        x2 = lax.rem(x + dx, NX)
        return x2 // 2, {"ep_0": x2 // 2, "rep_0": lax.rem(x2, 2)}

    def zc(dz, dc):
        z2, c2 = lax.rem(z + dz, NZ), lax.rem(core + dc, NC)
        return z2 * NC + c2, {"ep_1": z2, "ep_2": c2}

    def owner(dxh, dz, dc):
        h2, z2, c2 = lax.rem(xhi + dxh, 2), lax.rem(z + dz, NZ), lax.rem(core + dc, NC)
        return h2 * NC + c2, c2, {"ep_0": h2, "ep_1": z2, "ep_2": c2}

    def send(src, dst, send_sem, recv_sem, dev):
        pltpu.make_async_remote_copy(
            src_ref=src, dst_ref=dst, send_sem=s_send.at[send_sem], recv_sem=recv_sem, device_id=dev,
            device_id_type=MESH,
        ).start()

    def keep(src, dst, sem):
        pltpu.make_async_copy(src, dst, sem).start()

    def wait(ref, sem):
        pltpu.make_async_copy(ref, ref, sem).wait()

    barrier = pltpu.get_barrier_semaphore()
    partners = [in_plane(dxl, dy)[2] for dy in range(NY) for dxl in range(2) if dxl or dy]
    partners += [zc(dz, dc)[1] for dz, dc in ZC]
    partners += [{"ep_0": 1 - xhi, "rep_0": 1 - xlo}]
    partners += [owner(1, dz, dc)[2] for dz in (0, 1, 7, 2, 6) for dc in range(2)]
    for dev in partners:
        pl.semaphore_signal(barrier, inc=1, device_id=dev, device_id_type=MESH)
    pl.semaphore_wait(barrier, len(partners))

    toward = [(g, (NY - GROUP_DY[g]) % NY, dxl) for g in range(NY) for dxl in (1, 0)]
    for g, dy, dxl in toward:
        if dxl or dy:
            send(meta_ref, meta.at[2, g * 2 + xlo], 0, s_meta.at[2], in_plane(dxl, dy)[2])
    keep(meta_ref, meta.at[2, xlo], s_meta.at[2])
    for g, dy, dxl in toward:
        x2, y2, dev = in_plane(dxl, dy)
        piece = og_ref.at[:, :, pl.ds(pl.multiple_of((x2 * NY + y2) * cols, 128), cols)]
        if dxl or dy:
            send(piece, graw.at[g, 2, xlo], 2 if g else 1, s_first.at[g], dev)
        else:
            keep(piece, graw.at[g, 2, xlo], s_first.at[g])

    half = NE * cap
    for c in range(CHUNKS):
        for i in range(2):
            sel = jnp.where(
                lax.broadcasted_iota(jnp.int32, (half, pairs), 0) + i * half == slot_ref[...], 1.0, 0.0
            ).astype(jnp.bfloat16)
            packed = jnp.dot(sel, hid_ref[:, c * step:(c + 1) * step], preferred_element_type=jnp.float32)
            hp[c, i] = packed.astype(jnp.bfloat16).reshape(NE, cap, step)

    def hid(c):
        for dz, dc in ZC:
            e, dev = zc(dz, dc)
            send(hp.at[c, :, e], hz.at[c, :, core, (2 - dz) % NZ], 3 if dz else 4, s_hz.at[c], dev)
        keep(hp.at[c, :, z * NC + core], hz.at[c, :, core, 2], s_hz.at[c])

    eye = jnp.where(
        lax.broadcasted_iota(jnp.int32, (256, 256), 0) == lax.broadcasted_iota(jnp.int32, (256, 256), 1), 1.0, 0.0
    ).astype(jnp.bfloat16)

    def turn(c):
        wait(hz.at[c], s_hz.at[c])
        for i in range(2):
            for f in range(0, step, 256):
                block = hz[c, i, :, :, :, f:f + 256].reshape(half, 256)
                turned = lax.dot_general(eye, block, (((1,), (1,)), ((), ())), preferred_element_type=jnp.float32)
                hzt[c, i, f:f + 256, :] = turned.astype(jnp.bfloat16)
        for dx in (1, 3, 2):
            h2, dev = along_x(dx)
            send(hzt.at[c, h2], ht.at[x, c], 5, s_hx.at[c], dev)
        keep(hzt.at[c, xhi], ht.at[x, c], s_hx.at[c])

    up, down = in_plane(0, 1)[2], in_plane(0, 3)[2]

    def row(c):
        own = ht.at[pl.ds(0, NX), c]
        wait(own, s_hx.at[c])
        send(own, ht.at[pl.ds(2 * NX, NX), c], 6, s_hy.at[0, c], up)
        send(own, ht.at[pl.ds(NX, NX), c], 6, s_hy.at[1, c], down)

    def relay(c):
        wait(ht.at[pl.ds(2 * NX, NX), c], s_hy.at[0, c])
        send(ht.at[pl.ds(2 * NX, 2), c], ht.at[pl.ds(3 * NX, 2), c], 7, s_hy.at[2, c], up)
        wait(ht.at[pl.ds(NX, NX), c], s_hy.at[1, c])
        send(ht.at[pl.ds(NX + 2, 2), c], ht.at[pl.ds(3 * NX + 2, 2), c], 7, s_hy.at[3, c], down)

    def routes(_):
        wait(meta.at[2], s_meta.at[2])
        for dz, at in ((1, 1), (7, 3), (2, 0), (6, 4)):
            send(meta.at[2], meta.at[at], 8, s_meta.at[at], zc(dz, 0)[1])
        total = meta[2, 0]
        for q in range(1, 2 * NY):
            total = total + meta[2, q]
        cnt[...] = total

    plus, minus = zc(1, 0)[1], zc(7, 0)[1]

    def raw(g):
        wait(graw.at[g, 2], s_first.at[g])
        send(graw.at[g, 2], graw.at[g, 1], 9, s_raw.at[g, 1], plus)
        send(graw.at[g, 2], graw.at[g, 3], 9, s_raw.at[g, 3], minus)

    def far(g):
        wait(graw.at[g, 1], s_raw.at[g, 1])
        send(graw.at[g, 1], graw.at[g, 0], 9, s_raw.at[g, 0], plus)
        wait(graw.at[g, 3], s_raw.at[g, 3])
        send(graw.at[g, 3], graw.at[g, 4], 9, s_raw.at[g, 4], minus)

    chip_rows = 2 * NC * cap

    def slots_of(count, z1, h2, z2):
        r = lax.broadcasted_iota(jnp.int32, (count, toks), 0)
        gap = half - NC * cap
        near = r + jnp.where(r >= NC * cap, gap, 0) + z * (NC * cap)
        if count == chip_rows:
            return near.astype(jnp.float32)
        s = r - chip_rows
        beyond = s + jnp.where(s >= NC * cap, gap, 0) + z1 * (NC * cap)
        last = s - chip_rows + h2 * half + z2 * (NC * cap)
        return jnp.where(r < chip_rows, near, jnp.where(s < chip_rows, beyond, last)).astype(jnp.float32)

    def pack(g):
        if g == 0:
            for at in (0, 1, 3, 4):
                wait(meta.at[at], s_meta.at[at])
        wait(graw.at[g, 0], s_raw.at[g, 0])
        wait(graw.at[g, 4], s_raw.at[g, 4])

        @pl.loop(0, 2)
        def _(xl):
            for at in range(NEAR):
                if at == 0:
                    rows = slots_of(chip_rows * 5 // 2, lax.rem(z + 1, NZ), xhi, lax.rem(z + 2, NZ))
                elif at == NEAR - 1:
                    rows = slots_of(chip_rows * 5 // 2, lax.rem(z + 7, NZ), 1 - xhi, lax.rem(z + 6, NZ))
                else:
                    rows = slots_of(chip_rows, 0, 0, 0)
                info = meta[at, g * 2 + xl]
                first = rows == info[0:1, :]
                second = rows == info[1:2, :]
                weights = jnp.where(first, info[2:3, :], jnp.where(second, info[3:4, :], 0.0))
                weight = jnp.sum(weights, axis=1, keepdims=True)
                sel = jnp.where(first | second, 1.0, 0.0).astype(jnp.bfloat16)
                packed = jnp.dot(sel, graw[g, at, xl].reshape(toks, cols), preferred_element_type=jnp.float32) * weight
                packed = packed.astype(jnp.bfloat16)
                gnear[g, :, xl, at] = packed[:chip_rows].reshape(2 * NC, cap, cols)
                if at == 0 or at == NEAR - 1:
                    gfar[g, at // 4, :, xl] = packed[chip_rows:].reshape(3 * NC, cap, cols)

        here = pl.ds(g * NX + xhi * 2, 2)
        for side, dz, at in ((0, 1, 7), (1, 7, 5)):
            for dxh in range(2):
                for dc in range(2):
                    d, _, dev = owner(dxh, dz, dc)
                    send(gfar.at[g, side, d], gall.at[here, core, at], 10, s_gz.at[g], dev)
        for side, dz in ((0, 2), (1, 6)):
            for dc in range(2):
                _, c2, dev = owner(side, dz, dc)
                send(gfar.at[g, side, 2 * NC + c2], gall.at[here, core, 6], 10, s_gz.at[g], dev)
        for dxh, dc in ((1, 0), (1, 1), (0, 1)):
            d, _, dev = owner(dxh, 0, dc)
            send(gnear.at[g, d], gall.at[here, core, pl.ds(0, NEAR)], 11, s_gz.at[g], dev)
        keep(gnear.at[g, xhi * NC + core], gall.at[here, core, pl.ds(0, NEAR)], s_gz.at[g])
        if g == 0:
            me = z * NC + core
            for dz, dc in ZC:
                send(cnt, cnt_all.at[me], 12, s_cnt.at[0], zc(dz, dc)[1])
            keep(cnt, cnt_all.at[me], s_cnt.at[0])
        if g == 1:
            wait(cnt_all, s_cnt.at[0])
            loads = cnt_all[0]
            for e in range(1, NE):
                loads = loads + cnt_all[e]
            cnt_x[0] = loads
        if g == 2:
            send(cnt_x.at[0], cnt_x.at[1], 13, s_cnt.at[1], owner(1, 0, 0)[2])

    ready = set()

    def mul(g, c0, c1):
        if g not in ready:
            ready.add(g)
            wait(gall.at[pl.ds(g * NX, NX)], s_gz.at[g])
        if g == NY - 1:
            for c in range(c0, c1):
                wait(ht.at[pl.ds(3 * NX, 2), c], s_hy.at[2, c])
                wait(ht.at[pl.ds(3 * NX + 2, 2), c], s_hy.at[3, c])

        @pl.loop(c0, c1)
        def _(c):
            at = pl.ds(pl.multiple_of(c * step, step), step)
            part = None
            for xs in range(NX):
                q = g * NX + xs
                term = jnp.dot(ht[q, c], gall[q].reshape(half, cols), preferred_element_type=jnp.float32)
                part = term if part is None else part + term
            if g == 0:
                acc[at, :] = part
            elif g < NY - 1:
                acc[at, :] += part
            else:
                out_ref[0, at, :] = (acc[at, :] + part).astype(out_ref.dtype)

    steps = dict(hid=hid, routes=routes, raw=raw, turn=turn, far=far, row=row, relay=relay, pack=pack, mul=mul)
    for name, *which in ORDER:
        steps[name](*which)

    wait(cnt_x.at[1], s_cnt.at[1])
    load_ref[...] = cnt_x[0] + cnt_x[1]

    sent = (
        meta.at[2, pl.ds(0, 7)], graw.at[0, 2, 0], graw.at[pl.ds(1, 3), 2], hz.at[:, :, :, pl.ds(0, 7)],
        hz.at[:, :, 0, 0], ht.at[pl.ds(0, 3)], ht.at[pl.ds(0, 2 * NX)], ht.at[pl.ds(0, NX)],
        meta.at[pl.ds(0, 4)], graw.at[:, pl.ds(0, 4)], gfar, gnear.at[:, pl.ds(0, 3)],
        cnt_all.at[pl.ds(0, NE - 1)], cnt_x.at[0],
    )
    for i, ref in enumerate(sent):
        wait(ref, s_send.at[i])


def body(hidden, out_grad, route_weight, expert_ids):
    micro, tokens, picks, ff = hidden.shape
    width = out_grad.shape[2]
    experts = lax.axis_size(EP)
    replicas = lax.axis_size(REP)
    cols = width // replicas
    limit = 2 * tokens * picks // experts
    cap = micro * limit
    toks = micro * tokens
    ids = expert_ids.reshape(micro, tokens * picks)
    order = jnp.arange(tokens * picks, dtype=jnp.int32)
    earlier = (ids[:, :, None] == ids[:, None, :]) & (order[None, None, :] < order[None, :, None])
    position = jnp.sum(earlier.astype(jnp.int32), axis=2)
    slot = ids * cap + jnp.arange(micro, dtype=jnp.int32)[:, None] * limit + position
    by_token = slot.reshape(toks, picks).T.astype(jnp.float32)
    weights = route_weight.reshape(toks, picks).T
    tally = jnp.sum(
        (expert_ids.reshape(toks * picks)[None, :] == jnp.arange(toks, dtype=jnp.int32)[:, None]).astype(jnp.float32),
        axis=1,
    )
    meta = jnp.concatenate([by_token, weights, tally[None, :], jnp.zeros((3, toks), jnp.float32)], axis=0)
    vmem = pl.BlockSpec(memory_space=pltpu.VMEM)
    bf16 = jnp.bfloat16
    dma = pltpu.SemaphoreType.DMA
    grad, load = pl.pallas_call(
        kernel,
        out_shape=(
            jax.ShapeDtypeStruct((1, ff, cols), bf16),
            jax.ShapeDtypeStruct((8, toks), jnp.float32),
        ),
        in_specs=[vmem, vmem, vmem, pl.BlockSpec(memory_space=pl.ANY)],
        out_specs=(vmem, vmem),
        scratch_shapes=[
            pltpu.VMEM((NY, NEAR, 2, micro, tokens, cols), bf16),
            pltpu.VMEM((NEAR, 2 * NY, 8, toks), jnp.float32),
            pltpu.VMEM((NY, 2 * NC, 2, NEAR, cap, cols), bf16),
            pltpu.VMEM((NY, 2, 3 * NC, 2, cap, cols), bf16),
            pltpu.VMEM((NQ, NC, NZ, cap, cols), bf16),
            pltpu.VMEM((CHUNKS, 2, NE, cap, ff // CHUNKS), bf16),
            pltpu.VMEM((CHUNKS, 2, NC, NZ, cap, ff // CHUNKS), bf16),
            pltpu.VMEM((CHUNKS, 2, ff // CHUNKS, NE * cap), bf16),
            pltpu.VMEM((NQ, CHUNKS, ff // CHUNKS, NE * cap), bf16),
            pltpu.VMEM((ff, cols), jnp.float32),
            pltpu.VMEM((8, toks), jnp.float32),
            pltpu.VMEM((NE, 8, toks), jnp.float32),
            pltpu.VMEM((2, 8, toks), jnp.float32),
            dma((14,)),
            dma((NEAR,)),
            dma((NY,)),
            dma((NY, NEAR)),
            dma((NY,)),
            dma((CHUNKS,)),
            dma((CHUNKS,)),
            dma((4, CHUNKS)),
            dma((2,)),
        ],
        compiler_params=pltpu.CompilerParams(
            collective_id=0, has_side_effects=True, vmem_limit_bytes=67_000_000 // 1024 * 1024
        ),
    )(hidden.reshape(toks * picks, ff), slot.reshape(1, toks * picks), meta, out_grad)
    expert_load = load[4, :experts] / float(micro * tokens * replicas * picks)
    return grad, expert_load


def solution(mesh):
    finer = Mesh(mesh.devices.reshape(2, 4, 2, 8, 2), REP_EP)
    placed = (
        P(None, REP_EP, None, None),
        P(None, REP_EP, None),
        P(None, REP_EP, None),
        P(None, REP_EP, None),
    )
    return jax.shard_map(
        body, mesh=finer, in_specs=placed, out_specs=(P(EP, None, REP), P()), check_vma=False
    )
```

```python
import functools

import jax
import jax.numpy as jnp
from jax import lax
from jax.experimental import pallas as pl
from jax.experimental.pallas import tpu as pltpu
from jax.sharding import Mesh
from jax.sharding import PartitionSpec as P

REP_EP = ("rep_0", "rep_1", "ep_0", "ep_1", "ep_2")
EP = ("ep_0", "ep_1", "ep_2")
REP = ("rep_0", "rep_1")
MESH = pl.DeviceIdType.MESH
NX, NY, NZ, NC = 4, 4, 8, 2
NE = NZ * NC
NQ = NX * NY
NEAR = 5
CHUNKS = 8
ZC = [(1, 0), (7, 0), (1, 1), (7, 1), (2, 0), (6, 0), (2, 1), (6, 1), (3, 0), (5, 0), (3, 1), (5, 1), (4, 0), (4, 1), (0, 1)]
GROUP_DY = [0, 1, 3, 2]
ORDER = [
    ("fill", 0), ("hid", 0), ("fill", 3), ("fill", 5), ("fill", 4), ("fill", 6), ("hid", 5), ("turn", 0), ("fill", 2),
    ("routes", 0), ("hid", 4), ("hid", 6), ("turn", 5), ("late", 0), ("hid", 3), ("fill", 7), ("row", 0), ("hid", 7),
    ("count", 0), ("fill", 1), ("hid", 2), ("row", 5), ("hid", 1), ("turn", 3), ("turn", 7), ("turn", 4), ("raw", 1),
    ("relay", 0), ("raw", 0), ("turn", 6), ("raw", 3), ("row", 3), ("row", 6), ("turn", 2), ("turn", 1), ("far", 0),
    ("raw", 2), ("row", 7), ("near", 0), ("relay", 6), ("pack", 0), ("far", 1), ("row", 1), ("near", 1), ("far", 2),
    ("far", 3), ("row", 4), ("near", 2), ("row", 2), ("relay", 5), ("mul", 0, 0, 4), ("relay", 1), ("near", 3),
    ("mul", 0, 4, 8), ("pack", 1), ("pack", 2), ("pack", 3), ("relay", 2), ("relay", 3), ("relay", 7), ("relay", 4),
    ("mul", 1, 4, 8), ("count", 1), ("mul", 2, 4, 8), ("mul", 1, 0, 4), ("mul", 2, 0, 4), ("count", 2),
    ("mul", 3, 0, 4), ("mul", 3, 4, 8),
]


def kernel(hid_ref, slot_ref, meta_ref, og_ref, out_ref, load_ref,
           graw, meta, gnear, gfar, gall, hp, hz, hzt, ht, acc, cnt, cnt_all, cnt_x,
           s_send, s_meta, s_first, s_raw, s_gz, s_hz, s_hx, s_hy, s_cnt):
    cap, step = hp.shape[3], hp.shape[4]
    cols = graw.shape[5]
    toks = graw.shape[3] * graw.shape[4]
    pairs = hid_ref.shape[0]
    xlo, y = lax.axis_index("rep_0"), lax.axis_index("rep_1")
    xhi, z, core = lax.axis_index("ep_0"), lax.axis_index("ep_1"), lax.axis_index("ep_2")
    x = xhi * 2 + xlo

    def in_plane(dxl, dy):
        x2, y2 = lax.rem(xlo + dxl, 2), lax.rem(y + dy, NY)
        return x2, y2, {"rep_0": x2, "rep_1": y2}

    def along_x(dx):
        x2 = lax.rem(x + dx, NX)
        return x2 // 2, {"ep_0": x2 // 2, "rep_0": lax.rem(x2, 2)}

    def zc(dz, dc):
        z2, c2 = lax.rem(z + dz, NZ), lax.rem(core + dc, NC)
        return z2 * NC + c2, {"ep_1": z2, "ep_2": c2}

    def owner(dxh, dz, dc):
        h2, z2, c2 = lax.rem(xhi + dxh, 2), lax.rem(z + dz, NZ), lax.rem(core + dc, NC)
        return h2 * NC + c2, c2, {"ep_0": h2, "ep_1": z2, "ep_2": c2}

    def send(src, dst, send_sem, recv_sem, dev):
        pltpu.make_async_remote_copy(
            src_ref=src, dst_ref=dst, send_sem=s_send.at[send_sem], recv_sem=recv_sem, device_id=dev,
            device_id_type=MESH,
        ).start()

    def keep(src, dst, sem):
        pltpu.make_async_copy(src, dst, sem).start()

    def wait(ref, sem):
        pltpu.make_async_copy(ref, ref, sem).wait()

    barrier = pltpu.get_barrier_semaphore()
    partners = [in_plane(dxl, dy)[2] for dy in range(NY) for dxl in range(2) if dxl or dy]
    partners += [zc(dz, dc)[1] for dz, dc in ZC]
    partners += [{"ep_0": 1 - xhi, "rep_0": 1 - xlo}]
    partners += [owner(1, dz, dc)[2] for dz in (0, 1, 7, 2, 6) for dc in range(2)]
    for dev in partners:
        pl.semaphore_signal(barrier, inc=1, device_id=dev, device_id_type=MESH)
    pl.semaphore_wait(barrier, len(partners))

    toward = [(g, (NY - GROUP_DY[g]) % NY, dxl) for g in range(NY) for dxl in (1, 0)]
    for g, dy, dxl in toward:
        if dxl or dy:
            send(meta_ref, meta.at[2, g * 2 + xlo], 0, s_meta.at[2], in_plane(dxl, dy)[2])
    keep(meta_ref, meta.at[2, xlo], s_meta.at[2])

    def first(g, dy, dxl):
        x2, y2, dev = in_plane(dxl, dy)
        piece = og_ref.at[:, :, pl.ds(pl.multiple_of((x2 * NY + y2) * cols, 128), cols)]
        if dxl or dy:
            send(piece, graw.at[g, 2, xlo], 2 if g else 1, s_first.at[g], dev)
        else:
            keep(piece, graw.at[g, 2, xlo], s_first.at[g])

    for which in toward:
        if which[0] < 2 or not which[2]:
            first(*which)

    def late(_):
        for which in toward:
            if which[0] >= 2 and which[2]:
                first(*which)

    half = NE * cap

    def fill(c):
        for i in range(2):
            sel = jnp.where(
                lax.broadcasted_iota(jnp.int32, (half, pairs), 0) + i * half == slot_ref[...], 1.0, 0.0
            ).astype(jnp.bfloat16)
            packed = jnp.dot(sel, hid_ref[:, c * step:(c + 1) * step], preferred_element_type=jnp.float32)
            hp[c, i] = packed.astype(jnp.bfloat16).reshape(NE, cap, step)

    def hid(c):
        for dz, dc in ZC:
            e, dev = zc(dz, dc)
            send(hp.at[c, :, e], hz.at[c, :, core, (2 - dz) % NZ], 3 if dz else 4, s_hz.at[c], dev)
        keep(hp.at[c, :, z * NC + core], hz.at[c, :, core, 2], s_hz.at[c])

    eye = jnp.where(
        lax.broadcasted_iota(jnp.int32, (256, 256), 0) == lax.broadcasted_iota(jnp.int32, (256, 256), 1), 1.0, 0.0
    ).astype(jnp.bfloat16)

    def turn(c):
        wait(hz.at[c], s_hz.at[c])
        for i in range(2):
            for f in range(0, step, 256):
                block = hz[c, i, :, :, :, f:f + 256].reshape(half, 256)
                turned = lax.dot_general(eye, block, (((1,), (1,)), ((), ())), preferred_element_type=jnp.float32)
                hzt[c, i, f:f + 256, :] = turned.astype(jnp.bfloat16)
        for dx in (1, 3, 2):
            h2, dev = along_x(dx)
            send(hzt.at[c, h2], ht.at[x, c], 5, s_hx.at[c], dev)
        keep(hzt.at[c, xhi], ht.at[x, c], s_hx.at[c])

    up, down = in_plane(0, 1)[2], in_plane(0, 3)[2]

    def row(c):
        own = ht.at[pl.ds(0, NX), c]
        wait(own, s_hx.at[c])
        send(own, ht.at[pl.ds(2 * NX, NX), c], 6, s_hy.at[0, c], up)
        send(own, ht.at[pl.ds(NX, NX), c], 6, s_hy.at[1, c], down)

    def relay(c):
        wait(ht.at[pl.ds(2 * NX, NX), c], s_hy.at[0, c])
        send(ht.at[pl.ds(2 * NX, 2), c], ht.at[pl.ds(3 * NX, 2), c], 7, s_hy.at[2, c], up)
        wait(ht.at[pl.ds(NX, NX), c], s_hy.at[1, c])
        send(ht.at[pl.ds(NX + 2, 2), c], ht.at[pl.ds(3 * NX + 2, 2), c], 7, s_hy.at[3, c], down)

    def routes(_):
        wait(meta.at[2], s_meta.at[2])
        for dz, at in ((1, 1), (7, 3), (2, 0), (6, 4)):
            send(meta.at[2], meta.at[at], 8, s_meta.at[at], zc(dz, 0)[1])
        total = meta[2, 0]
        for q in range(1, 2 * NY):
            total = total + meta[2, q]
        cnt[...] = total

    plus, minus = zc(1, 0)[1], zc(7, 0)[1]

    def raw(g):
        wait(graw.at[g, 2], s_first.at[g])
        send(graw.at[g, 2], graw.at[g, 1], 9, s_raw.at[g, 1], plus)
        send(graw.at[g, 2], graw.at[g, 3], 9, s_raw.at[g, 3], minus)

    def far(g):
        wait(graw.at[g, 1], s_raw.at[g, 1])
        send(graw.at[g, 1], graw.at[g, 0], 9, s_raw.at[g, 0], plus)
        wait(graw.at[g, 3], s_raw.at[g, 3])
        send(graw.at[g, 3], graw.at[g, 4], 9, s_raw.at[g, 4], minus)

    chip_rows = 2 * NC * cap

    def slots_of(count, z1, h2, z2):
        r = lax.broadcasted_iota(jnp.int32, (count, toks), 0)
        gap = half - NC * cap
        near = r + jnp.where(r >= NC * cap, gap, 0) + z * (NC * cap)
        if count == chip_rows:
            return near.astype(jnp.float32)
        s = r - chip_rows
        beyond = s + jnp.where(s >= NC * cap, gap, 0) + z1 * (NC * cap)
        last = s - chip_rows + h2 * half + z2 * (NC * cap)
        return jnp.where(r < chip_rows, near, jnp.where(s < chip_rows, beyond, last)).astype(jnp.float32)

    def into_slots(g, sources):
        @pl.loop(0, 2)
        def _(xl):
            for at in sources:
                if at == 0:
                    rows = slots_of(chip_rows * 5 // 2, lax.rem(z + 1, NZ), xhi, lax.rem(z + 2, NZ))
                elif at == NEAR - 1:
                    rows = slots_of(chip_rows * 5 // 2, lax.rem(z + 7, NZ), 1 - xhi, lax.rem(z + 6, NZ))
                else:
                    rows = slots_of(chip_rows, 0, 0, 0)
                info = meta[at, g * 2 + xl]
                first = rows == info[0:1, :]
                second = rows == info[1:2, :]
                weights = jnp.where(first, info[2:3, :], jnp.where(second, info[3:4, :], 0.0))
                weight = jnp.sum(weights, axis=1, keepdims=True)
                sel = jnp.where(first | second, 1.0, 0.0).astype(jnp.bfloat16)
                packed = jnp.dot(sel, graw[g, at, xl].reshape(toks, cols), preferred_element_type=jnp.float32) * weight
                packed = packed.astype(jnp.bfloat16)
                gnear[g, :, xl, at] = packed[:chip_rows].reshape(2 * NC, cap, cols)
                if at == 0 or at == NEAR - 1:
                    gfar[g, at // 4, :, xl] = packed[chip_rows:].reshape(3 * NC, cap, cols)

    def to_owners(g, first, count):
        here, some = pl.ds(g * NX + xhi * 2, 2), pl.ds(first, count)
        for dxh, dc in ((1, 0), (1, 1), (0, 1)):
            d, _, dev = owner(dxh, 0, dc)
            send(gnear.at[g, d, :, some], gall.at[here, core, some], 11, s_gz.at[g], dev)
        keep(gnear.at[g, xhi * NC + core, :, some], gall.at[here, core, some], s_gz.at[g])

    seen = set()

    def known(offsets):
        for at in offsets:
            if at not in seen:
                seen.add(at)
                wait(meta.at[at], s_meta.at[at])

    def near(g):
        known((1, 3))
        into_slots(g, (1, 2, 3))
        to_owners(g, 1, 3)

    def pack(g):
        known((0, 4))
        wait(graw.at[g, 0], s_raw.at[g, 0])
        wait(graw.at[g, 4], s_raw.at[g, 4])
        into_slots(g, (0, 4))
        here = pl.ds(g * NX + xhi * 2, 2)
        for side, dz, at in ((0, 1, 7), (1, 7, 5)):
            for dxh in range(2):
                for dc in range(2):
                    d, _, dev = owner(dxh, dz, dc)
                    send(gfar.at[g, side, d], gall.at[here, core, at], 10, s_gz.at[g], dev)
        for side, dz in ((0, 2), (1, 6)):
            for dc in range(2):
                _, c2, dev = owner(side, dz, dc)
                send(gfar.at[g, side, 2 * NC + c2], gall.at[here, core, 6], 10, s_gz.at[g], dev)
        to_owners(g, 0, 1)
        to_owners(g, 4, 1)

    def count(part):
        if part == 0:
            me = z * NC + core
            for dz, dc in ZC:
                send(cnt, cnt_all.at[me], 12, s_cnt.at[0], zc(dz, dc)[1])
            keep(cnt, cnt_all.at[me], s_cnt.at[0])
            return
        if part == 2:
            send(cnt_x.at[0], cnt_x.at[1], 13, s_cnt.at[1], owner(1, 0, 0)[2])
            return
        wait(cnt_all, s_cnt.at[0])
        loads = cnt_all[0]
        for e in range(1, NE):
            loads = loads + cnt_all[e]
        cnt_x[0] = loads

    ready = set()

    def mul(g, c0, c1):
        if g not in ready:
            ready.add(g)
            wait(gall.at[pl.ds(g * NX, NX)], s_gz.at[g])
        if g == NY - 1:
            for c in range(c0, c1):
                wait(ht.at[pl.ds(3 * NX, 2), c], s_hy.at[2, c])
                wait(ht.at[pl.ds(3 * NX + 2, 2), c], s_hy.at[3, c])

        @pl.loop(c0, c1)
        def _(c):
            at = pl.ds(pl.multiple_of(c * step, step), step)
            part = None
            for xs in range(NX):
                q = g * NX + xs
                term = jnp.dot(ht[q, c], gall[q].reshape(half, cols), preferred_element_type=jnp.float32)
                part = term if part is None else part + term
            if g == 0:
                acc[at, :] = part
            elif g < NY - 1:
                acc[at, :] += part
            else:
                out_ref[0, at, :] = (acc[at, :] + part).astype(out_ref.dtype)

    steps = dict(fill=fill, late=late, near=near, count=count, hid=hid, routes=routes, raw=raw, turn=turn, far=far, row=row, relay=relay, pack=pack, mul=mul)
    for name, *which in ORDER:
        steps[name](*which)

    wait(cnt_x.at[1], s_cnt.at[1])
    load_ref[...] = cnt_x[0] + cnt_x[1]

    sent = (
        meta.at[2, pl.ds(0, 7)], graw.at[0, 2, 0], graw.at[pl.ds(1, 3), 2], hz.at[:, :, :, pl.ds(0, 7)],
        hz.at[:, :, 0, 0], ht.at[pl.ds(0, 3)], ht.at[pl.ds(0, 2 * NX)], ht.at[pl.ds(0, NX)],
        meta.at[pl.ds(0, 4)], graw.at[:, pl.ds(0, 4)], gfar, gnear.at[:, pl.ds(0, 3)],
        cnt_all.at[pl.ds(0, NE - 1)], cnt_x.at[0],
    )
    for i, ref in enumerate(sent):
        wait(ref, s_send.at[i])


def body(hidden, out_grad, route_weight, expert_ids):
    micro, tokens, picks, ff = hidden.shape
    width = out_grad.shape[2]
    experts = lax.axis_size(EP)
    replicas = lax.axis_size(REP)
    cols = width // replicas
    limit = 2 * tokens * picks // experts
    cap = micro * limit
    toks = micro * tokens
    ids = expert_ids.reshape(micro, tokens * picks)
    order = jnp.arange(tokens * picks, dtype=jnp.int32)
    earlier = (ids[:, :, None] == ids[:, None, :]) & (order[None, None, :] < order[None, :, None])
    position = jnp.sum(earlier.astype(jnp.int32), axis=2)
    slot = ids * cap + jnp.arange(micro, dtype=jnp.int32)[:, None] * limit + position
    by_token = slot.reshape(toks, picks).T.astype(jnp.float32)
    weights = route_weight.reshape(toks, picks).T
    tally = jnp.sum(
        (expert_ids.reshape(toks * picks)[None, :] == jnp.arange(toks, dtype=jnp.int32)[:, None]).astype(jnp.float32),
        axis=1,
    )
    meta = jnp.concatenate([by_token, weights, tally[None, :], jnp.zeros((3, toks), jnp.float32)], axis=0)
    vmem = pl.BlockSpec(memory_space=pltpu.VMEM)
    bf16 = jnp.bfloat16
    dma = pltpu.SemaphoreType.DMA
    grad, load = pl.pallas_call(
        kernel,
        out_shape=(
            jax.ShapeDtypeStruct((1, ff, cols), bf16),
            jax.ShapeDtypeStruct((8, toks), jnp.float32),
        ),
        in_specs=[vmem, vmem, vmem, pl.BlockSpec(memory_space=pl.ANY)],
        out_specs=(vmem, vmem),
        scratch_shapes=[
            pltpu.VMEM((NY, NEAR, 2, micro, tokens, cols), bf16),
            pltpu.VMEM((NEAR, 2 * NY, 8, toks), jnp.float32),
            pltpu.VMEM((NY, 2 * NC, 2, NEAR, cap, cols), bf16),
            pltpu.VMEM((NY, 2, 3 * NC, 2, cap, cols), bf16),
            pltpu.VMEM((NQ, NC, NZ, cap, cols), bf16),
            pltpu.VMEM((CHUNKS, 2, NE, cap, ff // CHUNKS), bf16),
            pltpu.VMEM((CHUNKS, 2, NC, NZ, cap, ff // CHUNKS), bf16),
            pltpu.VMEM((CHUNKS, 2, ff // CHUNKS, NE * cap), bf16),
            pltpu.VMEM((NQ, CHUNKS, ff // CHUNKS, NE * cap), bf16),
            pltpu.VMEM((ff, cols), jnp.float32),
            pltpu.VMEM((8, toks), jnp.float32),
            pltpu.VMEM((NE, 8, toks), jnp.float32),
            pltpu.VMEM((2, 8, toks), jnp.float32),
            dma((14,)),
            dma((NEAR,)),
            dma((NY,)),
            dma((NY, NEAR)),
            dma((NY,)),
            dma((CHUNKS,)),
            dma((CHUNKS,)),
            dma((4, CHUNKS)),
            dma((2,)),
        ],
        compiler_params=pltpu.CompilerParams(
            collective_id=0, has_side_effects=True, vmem_limit_bytes=67_000_000 // 1024 * 1024
        ),
    )(hidden.reshape(toks * picks, ff), slot.reshape(1, toks * picks), meta, out_grad)
    expert_load = load[4, :experts] / float(micro * tokens * replicas * picks)
    return grad, expert_load


def solution(mesh):
    finer = Mesh(mesh.devices.reshape(2, 4, 2, 8, 2), REP_EP)
    placed = (
        P(None, REP_EP, None, None),
        P(None, REP_EP, None),
        P(None, REP_EP, None),
        P(None, REP_EP, None),
    )
    return jax.shard_map(
        body, mesh=finer, in_specs=placed, out_specs=(P(EP, None, REP), P()), check_vma=False
    )
```

```python
import functools

import jax
import jax.numpy as jnp
from jax import lax
from jax.experimental import pallas as pl
from jax.experimental.pallas import tpu as pltpu
from jax.sharding import Mesh
from jax.sharding import PartitionSpec as P

REP_EP = ("rep_0", "rep_1", "ep_0", "ep_1", "ep_2")
EP = ("ep_0", "ep_1", "ep_2")
REP = ("rep_0", "rep_1")
MESH = pl.DeviceIdType.MESH
NX, NY, NZ, NC = 4, 4, 8, 2
NE = NZ * NC
NQ = NX * NY
NEAR = 5
CHUNKS = 8
ZC = [(1, 0), (7, 0), (1, 1), (7, 1), (2, 0), (6, 0), (2, 1), (6, 1), (3, 0), (5, 0), (3, 1), (5, 1), (4, 0), (4, 1), (0, 1)]
GROUP_DY = [0, 1, 3, 2]
EARLY = [
    ("fill", 0), ("fill", 1), ("fill", 2), ("fill", 3), ("fill", 4), ("fill", 5), ("fill", 6), ("fill", 7),
]
ORDER = [
    ("hid", 0), ("hid", 5), ("turn", 0), ("routes", 0), ("hid", 4), ("hid", 6), ("turn", 5), ("late", 0), ("hid", 3),
    ("row", 0), ("hid", 7), ("count", 0), ("hid", 2), ("row", 5), ("hid", 1), ("turn", 3), ("turn", 7), ("turn", 4),
    ("raw", 1), ("relay", 0), ("raw", 0), ("turn", 6), ("raw", 3), ("row", 3), ("row", 6), ("turn", 2), ("turn", 1),
    ("far", 0), ("raw", 2), ("row", 7), ("near", 0), ("relay", 6), ("pack", 0), ("far", 1), ("row", 1), ("near", 1),
    ("far", 2), ("far", 3), ("row", 4), ("near", 2), ("row", 2), ("relay", 5), ("mul", 0, 0, 4), ("relay", 1),
    ("near", 3), ("mul", 0, 4, 8), ("pack", 1), ("pack", 2), ("pack", 3), ("relay", 2), ("relay", 3), ("relay", 7),
    ("relay", 4), ("mul", 1, 4, 8), ("count", 1), ("mul", 2, 4, 8), ("mul", 1, 0, 4), ("mul", 2, 0, 4), ("count", 2),
    ("mul", 3, 0, 4), ("mul", 3, 4, 8),
]


def kernel(limit, total_pairs, hid_ref, ids_ref, weight_ref, og_ref, out_ref, load_ref,
           meta_ref, pair_slot, graw, meta, gnear, gfar, gall, hp, hz, hzt, ht, acc, cnt, cnt_all, cnt_x,
           s_send, s_meta, s_first, s_raw, s_gz, s_hz, s_hx, s_hy, s_cnt):
    cap, step = hp.shape[3], hp.shape[4]
    cols = graw.shape[5]
    toks = graw.shape[3] * graw.shape[4]
    micro, tokens, picks = hid_ref.shape[:3]
    pairs = toks * picks
    half = NE * cap
    f32, bf16, i32 = jnp.float32, jnp.bfloat16, jnp.int32
    xlo, y = lax.axis_index("rep_0"), lax.axis_index("rep_1")
    xhi, z, core = lax.axis_index("ep_0"), lax.axis_index("ep_1"), lax.axis_index("ep_2")
    x = xhi * 2 + xlo

    def in_plane(dxl, dy):
        x2, y2 = lax.rem(xlo + dxl, 2), lax.rem(y + dy, NY)
        return x2, y2, {"rep_0": x2, "rep_1": y2}

    def along_x(dx):
        x2 = lax.rem(x + dx, NX)
        return x2 // 2, {"ep_0": x2 // 2, "rep_0": lax.rem(x2, 2)}

    def zc(dz, dc):
        z2, c2 = lax.rem(z + dz, NZ), lax.rem(core + dc, NC)
        return z2 * NC + c2, {"ep_1": z2, "ep_2": c2}

    def owner(dxh, dz, dc):
        h2, z2, c2 = lax.rem(xhi + dxh, 2), lax.rem(z + dz, NZ), lax.rem(core + dc, NC)
        return h2 * NC + c2, c2, {"ep_0": h2, "ep_1": z2, "ep_2": c2}

    def send(src, dst, send_sem, recv_sem, dev):
        pltpu.make_async_remote_copy(
            src_ref=src, dst_ref=dst, send_sem=s_send.at[send_sem], recv_sem=recv_sem, device_id=dev,
            device_id_type=MESH,
        ).start()

    def keep(src, dst, sem):
        pltpu.make_async_copy(src, dst, sem).start()

    def wait(ref, sem):
        pltpu.make_async_copy(ref, ref, sem).wait()

    barrier = pltpu.get_barrier_semaphore()
    partners = [in_plane(dxl, dy)[2] for dy in range(NY) for dxl in range(2) if dxl or dy]
    partners += [zc(dz, dc)[1] for dz, dc in ZC]
    partners += [{"ep_0": 1 - xhi, "rep_0": 1 - xlo}]
    partners += [owner(1, dz, dc)[2] for dz in (0, 1, 7, 2, 6) for dc in range(2)]
    for dev in partners:
        pl.semaphore_signal(barrier, inc=1, device_id=dev, device_id_type=MESH)

    def across(ref, k):
        return jnp.concatenate([ref[m, k:k + 1, :] for m in range(micro)], axis=1)

    def square(rows):
        return lax.broadcasted_iota(i32, (rows, toks), 0), lax.broadcasted_iota(i32, (rows, toks), 1)

    down_at, along_at = square(toks)
    same = down_at // tokens == along_at // tokens
    block = jnp.where(same, 1.0, 0.0).astype(bf16)
    before = jnp.where(same & (down_at < along_at), 1.0, 0.0).astype(bf16)
    ids = [across(ids_ref, k) for k in range(picks)]
    hits = [jnp.where(down_at == e, 1.0, 0.0).astype(bf16) for e in ids]
    lane_micro = (lax.broadcasted_iota(i32, (1, toks), 1) // tokens).astype(f32)
    within, passed = [], None
    for hit in hits:
        earlier = jnp.dot(hit, before, preferred_element_type=f32)
        if passed is not None:
            earlier = earlier + jnp.dot(passed, block, preferred_element_type=f32)
        place = jnp.sum(hit.astype(f32) * earlier, axis=0, keepdims=True)
        within.append(lane_micro * limit + place)
        passed = hit if passed is None else passed + hit
    tally = lax.dot_general(
        jnp.ones((8, toks), bf16), passed, (((1,), (1,)), ((), ())), preferred_element_type=f32
    )[0:1, :]
    rows = [ids[k].astype(f32) * cap + within[k] for k in range(picks)]
    rows += [across(weight_ref, k) for k in range(picks)] + [tally]
    line = lax.broadcasted_iota(i32, (8, toks), 0)
    own_meta = jnp.zeros((8, toks), f32)
    for i, row_of in enumerate(rows):
        own_meta = jnp.where(line == i, row_of, own_meta)
    meta_ref[...] = own_meta
    spread = jnp.zeros((8, pairs), f32)
    eight = lax.broadcasted_iota(i32, (8, toks), 0)
    for k in range(picks):
        put = jnp.where(
            lax.broadcasted_iota(i32, (toks, pairs), 1) == lax.broadcasted_iota(i32, (toks, pairs), 0) * picks + k, 1.0, 0.0
        ).astype(bf16)
        both = jnp.where(eight == 0, ids[k].astype(f32), within[k]).astype(bf16)
        spread = spread + jnp.dot(both, put, preferred_element_type=f32)
    pair_slot[...] = (spread[0:1, :] * cap + spread[1:2, :]).astype(i32)

    def fill(c):
        rows_here = hid_ref[:, :, :, c * step:(c + 1) * step].reshape(pairs, step)
        for i in range(2):
            sel = jnp.where(
                lax.broadcasted_iota(i32, (half, pairs), 0) + i * half == pair_slot[...], 1.0, 0.0
            ).astype(bf16)
            packed = jnp.dot(sel, rows_here, preferred_element_type=f32)
            hp[c, i] = packed.astype(bf16).reshape(NE, cap, step)

    for name, *which in EARLY:
        fill(*which)
    pl.semaphore_wait(barrier, len(partners))

    toward = [(g, (NY - GROUP_DY[g]) % NY, dxl) for g in range(NY) for dxl in (1, 0)]
    for g, dy, dxl in toward:
        if dxl or dy:
            send(meta_ref, meta.at[2, g * 2 + xlo], 0, s_meta.at[2], in_plane(dxl, dy)[2])
    keep(meta_ref, meta.at[2, xlo], s_meta.at[2])

    def first(g, dy, dxl):
        x2, y2, dev = in_plane(dxl, dy)
        piece = og_ref.at[:, :, pl.ds(pl.multiple_of((x2 * NY + y2) * cols, 128), cols)]
        if dxl or dy:
            send(piece, graw.at[g, 2, xlo], 2 if g else 1, s_first.at[g], dev)
        else:
            keep(piece, graw.at[g, 2, xlo], s_first.at[g])

    for which in toward:
        if which[0] < 2 or not which[2]:
            first(*which)

    def late(_):
        for which in toward:
            if which[0] >= 2 and which[2]:
                first(*which)

    def hid(c):
        for dz, dc in ZC:
            e, dev = zc(dz, dc)
            send(hp.at[c, :, e], hz.at[c, :, core, (2 - dz) % NZ], 3 if dz else 4, s_hz.at[c], dev)
        keep(hp.at[c, :, z * NC + core], hz.at[c, :, core, 2], s_hz.at[c])

    eye = jnp.where(
        lax.broadcasted_iota(jnp.int32, (256, 256), 0) == lax.broadcasted_iota(jnp.int32, (256, 256), 1), 1.0, 0.0
    ).astype(jnp.bfloat16)

    def turn(c):
        wait(hz.at[c], s_hz.at[c])
        for i in range(2):
            for f in range(0, step, 256):
                block = hz[c, i, :, :, :, f:f + 256].reshape(half, 256)
                turned = lax.dot_general(eye, block, (((1,), (1,)), ((), ())), preferred_element_type=jnp.float32)
                hzt[c, i, f:f + 256, :] = turned.astype(jnp.bfloat16)
        for dx in (1, 3, 2):
            h2, dev = along_x(dx)
            send(hzt.at[c, h2], ht.at[x, c], 5, s_hx.at[c], dev)
        keep(hzt.at[c, xhi], ht.at[x, c], s_hx.at[c])

    up, down = in_plane(0, 1)[2], in_plane(0, 3)[2]

    def row(c):
        own = ht.at[pl.ds(0, NX), c]
        wait(own, s_hx.at[c])
        send(own, ht.at[pl.ds(2 * NX, NX), c], 6, s_hy.at[0, c], up)
        send(own, ht.at[pl.ds(NX, NX), c], 6, s_hy.at[1, c], down)

    def relay(c):
        wait(ht.at[pl.ds(2 * NX, NX), c], s_hy.at[0, c])
        send(ht.at[pl.ds(2 * NX, 2), c], ht.at[pl.ds(3 * NX, 2), c], 7, s_hy.at[2, c], up)
        wait(ht.at[pl.ds(NX, NX), c], s_hy.at[1, c])
        send(ht.at[pl.ds(NX + 2, 2), c], ht.at[pl.ds(3 * NX + 2, 2), c], 7, s_hy.at[3, c], down)

    def routes(_):
        wait(meta.at[2], s_meta.at[2])
        for dz, at in ((1, 1), (7, 3), (2, 0), (6, 4)):
            send(meta.at[2], meta.at[at], 8, s_meta.at[at], zc(dz, 0)[1])
        total = meta[2, 0]
        for q in range(1, 2 * NY):
            total = total + meta[2, q]
        cnt[...] = total

    plus, minus = zc(1, 0)[1], zc(7, 0)[1]

    def raw(g):
        wait(graw.at[g, 2], s_first.at[g])
        send(graw.at[g, 2], graw.at[g, 1], 9, s_raw.at[g, 1], plus)
        send(graw.at[g, 2], graw.at[g, 3], 9, s_raw.at[g, 3], minus)

    def far(g):
        wait(graw.at[g, 1], s_raw.at[g, 1])
        send(graw.at[g, 1], graw.at[g, 0], 9, s_raw.at[g, 0], plus)
        wait(graw.at[g, 3], s_raw.at[g, 3])
        send(graw.at[g, 3], graw.at[g, 4], 9, s_raw.at[g, 4], minus)

    chip_rows = 2 * NC * cap

    def slots_of(count, z1, h2, z2):
        r = lax.broadcasted_iota(jnp.int32, (count, toks), 0)
        gap = half - NC * cap
        near = r + jnp.where(r >= NC * cap, gap, 0) + z * (NC * cap)
        if count == chip_rows:
            return near.astype(jnp.float32)
        s = r - chip_rows
        beyond = s + jnp.where(s >= NC * cap, gap, 0) + z1 * (NC * cap)
        last = s - chip_rows + h2 * half + z2 * (NC * cap)
        return jnp.where(r < chip_rows, near, jnp.where(s < chip_rows, beyond, last)).astype(jnp.float32)

    def into_slots(g, sources):
        @pl.loop(0, 2)
        def _(xl):
            for at in sources:
                if at == 0:
                    rows = slots_of(chip_rows * 5 // 2, lax.rem(z + 1, NZ), xhi, lax.rem(z + 2, NZ))
                elif at == NEAR - 1:
                    rows = slots_of(chip_rows * 5 // 2, lax.rem(z + 7, NZ), 1 - xhi, lax.rem(z + 6, NZ))
                else:
                    rows = slots_of(chip_rows, 0, 0, 0)
                info = meta[at, g * 2 + xl]
                first = rows == info[0:1, :]
                second = rows == info[1:2, :]
                weights = jnp.where(first, info[2:3, :], jnp.where(second, info[3:4, :], 0.0))
                weight = jnp.sum(weights, axis=1, keepdims=True)
                sel = jnp.where(first | second, 1.0, 0.0).astype(jnp.bfloat16)
                packed = jnp.dot(sel, graw[g, at, xl].reshape(toks, cols), preferred_element_type=jnp.float32) * weight
                packed = packed.astype(jnp.bfloat16)
                gnear[g, :, xl, at] = packed[:chip_rows].reshape(2 * NC, cap, cols)
                if at == 0 or at == NEAR - 1:
                    gfar[g, at // 4, :, xl] = packed[chip_rows:].reshape(3 * NC, cap, cols)

    def to_owners(g, first, count):
        here, some = pl.ds(g * NX + xhi * 2, 2), pl.ds(first, count)
        for dxh, dc in ((1, 0), (1, 1), (0, 1)):
            d, _, dev = owner(dxh, 0, dc)
            send(gnear.at[g, d, :, some], gall.at[here, core, some], 11, s_gz.at[g], dev)
        keep(gnear.at[g, xhi * NC + core, :, some], gall.at[here, core, some], s_gz.at[g])

    seen = set()

    def known(offsets):
        for at in offsets:
            if at not in seen:
                seen.add(at)
                wait(meta.at[at], s_meta.at[at])

    def near(g):
        known((1, 3))
        into_slots(g, (1, 2, 3))
        to_owners(g, 1, 3)

    def pack(g):
        known((0, 4))
        wait(graw.at[g, 0], s_raw.at[g, 0])
        wait(graw.at[g, 4], s_raw.at[g, 4])
        into_slots(g, (0, 4))
        here = pl.ds(g * NX + xhi * 2, 2)
        for side, dz, at in ((0, 1, 7), (1, 7, 5)):
            for dxh in range(2):
                for dc in range(2):
                    d, _, dev = owner(dxh, dz, dc)
                    send(gfar.at[g, side, d], gall.at[here, core, at], 10, s_gz.at[g], dev)
        for side, dz in ((0, 2), (1, 6)):
            for dc in range(2):
                _, c2, dev = owner(side, dz, dc)
                send(gfar.at[g, side, 2 * NC + c2], gall.at[here, core, 6], 10, s_gz.at[g], dev)
        to_owners(g, 0, 1)
        to_owners(g, 4, 1)

    def count(part):
        if part == 0:
            me = z * NC + core
            for dz, dc in ZC:
                send(cnt, cnt_all.at[me], 12, s_cnt.at[0], zc(dz, dc)[1])
            keep(cnt, cnt_all.at[me], s_cnt.at[0])
            return
        if part == 2:
            send(cnt_x.at[0], cnt_x.at[1], 13, s_cnt.at[1], owner(1, 0, 0)[2])
            return
        wait(cnt_all, s_cnt.at[0])
        loads = cnt_all[0]
        for e in range(1, NE):
            loads = loads + cnt_all[e]
        cnt_x[0] = loads

    ready = set()

    def mul(g, c0, c1):
        if g not in ready:
            ready.add(g)
            wait(gall.at[pl.ds(g * NX, NX)], s_gz.at[g])
        if g == NY - 1:
            for c in range(c0, c1):
                wait(ht.at[pl.ds(3 * NX, 2), c], s_hy.at[2, c])
                wait(ht.at[pl.ds(3 * NX + 2, 2), c], s_hy.at[3, c])

        @pl.loop(c0, c1)
        def _(c):
            at = pl.ds(pl.multiple_of(c * step, step), step)
            part = None
            for xs in range(NX):
                q = g * NX + xs
                term = jnp.dot(ht[q, c], gall[q].reshape(half, cols), preferred_element_type=jnp.float32)
                part = term if part is None else part + term
            if g == 0:
                acc[at, :] = part
            elif g < NY - 1:
                acc[at, :] += part
            else:
                out_ref[0, at, :] = (acc[at, :] + part).astype(out_ref.dtype)

    steps = dict(late=late, near=near, count=count, hid=hid, routes=routes, raw=raw, turn=turn, far=far, row=row, relay=relay, pack=pack, mul=mul)
    for name, *which in ORDER:
        steps[name](*which)

    wait(cnt_x.at[1], s_cnt.at[1])
    load_ref[...] = ((cnt_x[0, 4:5, :] + cnt_x[1, 4:5, :]) / total_pairs)[0, :load_ref.shape[0]]

    sent = (
        meta.at[2, pl.ds(0, 7)], graw.at[0, 2, 0], graw.at[pl.ds(1, 3), 2], hz.at[:, :, :, pl.ds(0, 7)],
        hz.at[:, :, 0, 0], ht.at[pl.ds(0, 3)], ht.at[pl.ds(0, 2 * NX)], ht.at[pl.ds(0, NX)],
        meta.at[pl.ds(0, 4)], graw.at[:, pl.ds(0, 4)], gfar, gnear.at[:, pl.ds(0, 3)],
        cnt_all.at[pl.ds(0, NE - 1)], cnt_x.at[0],
    )
    for i, ref in enumerate(sent):
        wait(ref, s_send.at[i])


def body(hidden, out_grad, route_weight, expert_ids):
    micro, tokens, picks, ff = hidden.shape
    width = out_grad.shape[2]
    experts = lax.axis_size(EP)
    replicas = lax.axis_size(REP)
    cols = width // replicas
    limit = 2 * tokens * picks // experts
    cap = micro * limit
    toks = micro * tokens
    vmem = pl.BlockSpec(memory_space=pltpu.VMEM)
    bf16 = jnp.bfloat16
    dma = pltpu.SemaphoreType.DMA
    grad, load = pl.pallas_call(
        functools.partial(kernel, limit, float(micro * tokens * replicas * picks)),
        out_shape=(
            pltpu.VMEM((1, ff, cols), bf16),
            pltpu.VMEM((experts,), jnp.float32),
        ),
        in_specs=[vmem, vmem, vmem, pl.BlockSpec(memory_space=pl.ANY)],
        out_specs=(vmem, vmem),
        scratch_shapes=[
            pltpu.VMEM((8, toks), jnp.float32),
            pltpu.VMEM((1, toks * picks), jnp.int32),
            pltpu.VMEM((NY, NEAR, 2, micro, tokens, cols), bf16),
            pltpu.VMEM((NEAR, 2 * NY, 8, toks), jnp.float32),
            pltpu.VMEM((NY, 2 * NC, 2, NEAR, cap, cols), bf16),
            pltpu.VMEM((NY, 2, 3 * NC, 2, cap, cols), bf16),
            pltpu.VMEM((NQ, NC, NZ, cap, cols), bf16),
            pltpu.VMEM((CHUNKS, 2, NE, cap, ff // CHUNKS), bf16),
            pltpu.VMEM((CHUNKS, 2, NC, NZ, cap, ff // CHUNKS), bf16),
            pltpu.VMEM((CHUNKS, 2, ff // CHUNKS, NE * cap), bf16),
            pltpu.VMEM((NQ, CHUNKS, ff // CHUNKS, NE * cap), bf16),
            pltpu.VMEM((ff, cols), jnp.float32),
            pltpu.VMEM((8, toks), jnp.float32),
            pltpu.VMEM((NE, 8, toks), jnp.float32),
            pltpu.VMEM((2, 8, toks), jnp.float32),
            dma((14,)),
            dma((NEAR,)),
            dma((NY,)),
            dma((NY, NEAR)),
            dma((NY,)),
            dma((CHUNKS,)),
            dma((CHUNKS,)),
            dma((4, CHUNKS)),
            dma((2,)),
        ],
        compiler_params=pltpu.CompilerParams(
            collective_id=0, has_side_effects=True, vmem_limit_bytes=62_000_000 // 1024 * 1024
        ),
    )(hidden, expert_ids.transpose(0, 2, 1), route_weight.transpose(0, 2, 1), out_grad)
    return grad, load


def solution(mesh):
    finer = Mesh(mesh.devices.reshape(2, 4, 2, 8, 2), REP_EP)
    placed = (
        P(None, REP_EP, None, None),
        P(None, REP_EP, None),
        P(None, REP_EP, None),
        P(None, REP_EP, None),
    )
    return jax.shard_map(
        body, mesh=finer, in_specs=placed, out_specs=(P(EP, None, REP), P()), check_vma=False
    )
```

```python
import functools

import jax
import jax.numpy as jnp
from jax import lax
from jax.experimental import pallas as pl
from jax.experimental.pallas import tpu as pltpu
from jax.sharding import Mesh
from jax.sharding import PartitionSpec as P

REP_EP = ("rep_0", "rep_1", "ep_0", "ep_1", "ep_2")
EP = ("ep_0", "ep_1", "ep_2")
REP = ("rep_0", "rep_1")
MESH = pl.DeviceIdType.MESH
NX, NY, NZ, NC = 4, 4, 8, 2
NE = NZ * NC
NQ = NX * NY
NEAR = 5
CHUNKS = 8
ZC = [(1, 0), (7, 0), (1, 1), (7, 1), (2, 0), (6, 0), (2, 1), (6, 1), (3, 0), (5, 0), (3, 1), (5, 1), (4, 0), (4, 1), (0, 1)]
GROUP_DY = [0, 1, 3, 2]
FIRST = 0
ORDER = [
    ("hid", 0), ("fill", 6), ("fill", 2), ("hid", 2), ("hid", 6), ("fill", 1), ("turn", 0), ("routes", 0), ("raw", 0),
    ("fill", 5), ("fill", 7), ("turn", 2), ("late", 0), ("row", 0), ("hid", 7), ("fill", 3), ("count", 0),
    ("turn", 6), ("raw", 1), ("raw", 2), ("row", 2), ("raw", 3), ("hid", 3), ("far", 0), ("near", 0), ("relay", 0),
    ("turn", 7), ("fill", 4), ("hid", 1), ("hid", 5), ("hid", 4), ("row", 6), ("far", 1), ("near", 1), ("far", 2),
    ("row", 7), ("near", 2), ("far", 3), ("near", 3), ("turn", 3), ("relay", 6), ("relay", 2), ("relay", 7),
    ("turn", 1), ("row", 3), ("turn", 5), ("pack", 0), ("turn", 4), ("row", 1), ("pack", 1), ("relay", 3), ("row", 5),
    ("pack", 2), ("pack", 3, 0), ("row", 4), ("relay", 5), ("pack", 3, 1), ("relay", 1), ("mul", 0, 4, 8),
    ("relay", 4), ("mul", 0, 0, 4), ("mul", 1, 0, 4), ("mul", 1, 4, 8), ("count", 1), ("mul", 2, 0, 4),
    ("mul", 2, 4, 8), ("mul", 3, 0, 4, 0), ("mul", 3, 4, 8, 0), ("count", 2), ("mul", 3, 0, 4, 1),
    ("mul", 3, 4, 8, 1),
]


def kernel(limit, total_pairs, hid_hbm, ids_hbm, weight_hbm, og_ref, out_ref, load_ref,
           hid_ref, ids_ref, weight_ref, meta_ref, pair_slot, graw, meta, near_meta, gnear, gfar, gall, hp, hz, hzt, ht, acc, cnt, cnt_all, cnt_x,
           s_send, s_meta, s_first, s_raw, s_gz, s_hz, s_hx, s_hy, s_cnt, s_own):
    cap, step = hp.shape[3], hp.shape[4]
    cols = graw.shape[5]
    toks = graw.shape[3] * graw.shape[4]
    micro, tokens, picks = hid_ref.shape[:3]
    pairs = toks * picks
    half = NE * cap
    f32, bf16, i32 = jnp.float32, jnp.bfloat16, jnp.int32
    xlo, y = lax.axis_index("rep_0"), lax.axis_index("rep_1")
    xhi, z, core = lax.axis_index("ep_0"), lax.axis_index("ep_1"), lax.axis_index("ep_2")
    x = xhi * 2 + xlo

    def in_plane(dxl, dy):
        x2, y2 = lax.rem(xlo + dxl, 2), lax.rem(y + dy, NY)
        return x2, y2, {"rep_0": x2, "rep_1": y2}

    def along_x(dx):
        x2 = lax.rem(x + dx, NX)
        return x2 // 2, {"ep_0": x2 // 2, "rep_0": lax.rem(x2, 2)}

    def zc(dz, dc):
        z2, c2 = lax.rem(z + dz, NZ), lax.rem(core + dc, NC)
        return z2 * NC + c2, {"ep_1": z2, "ep_2": c2}

    def owner(dxh, dz, dc):
        h2, z2, c2 = lax.rem(xhi + dxh, 2), lax.rem(z + dz, NZ), lax.rem(core + dc, NC)
        return h2 * NC + c2, c2, {"ep_0": h2, "ep_1": z2, "ep_2": c2}

    def send(src, dst, send_sem, recv_sem, dev):
        pltpu.make_async_remote_copy(
            src_ref=src, dst_ref=dst, send_sem=s_send.at[send_sem], recv_sem=recv_sem, device_id=dev,
            device_id_type=MESH,
        ).start()

    def keep(src, dst, sem):
        pltpu.make_async_copy(src, dst, sem).start()

    def wait(ref, sem):
        pltpu.make_async_copy(ref, ref, sem).wait()

    barrier = pltpu.get_barrier_semaphore()
    partners = [in_plane(dxl, dy)[2] for dy in range(NY) for dxl in range(2) if dxl or dy]
    partners += [zc(dz, dc)[1] for dz, dc in ZC]
    partners += [{"ep_0": 1 - xhi, "rep_0": 1 - xlo}]
    partners += [owner(1, dz, dc)[2] for dz in (0, 1, 7, 2, 6) for dc in range(2)]
    for dev in partners:
        pl.semaphore_signal(barrier, inc=1, device_id=dev, device_id_type=MESH)

    fetches = [
        pltpu.make_async_copy(src, dst, s_own.at[i])
        for i, (src, dst) in enumerate(((ids_hbm, ids_ref), (weight_hbm, weight_ref), (hid_hbm, hid_ref)))
    ]
    for fetch in fetches:
        fetch.start()
    for fetch in fetches[:2]:
        fetch.wait()

    def across(ref, k):
        return jnp.concatenate([ref[m, k:k + 1, :] for m in range(micro)], axis=1)

    def square(rows):
        return lax.broadcasted_iota(i32, (rows, toks), 0), lax.broadcasted_iota(i32, (rows, toks), 1)

    down_at, along_at = square(toks)
    same = down_at // tokens == along_at // tokens
    block = jnp.where(same, 1.0, 0.0).astype(bf16)
    before = jnp.where(same & (down_at < along_at), 1.0, 0.0).astype(bf16)
    ids = [across(ids_ref, k) for k in range(picks)]
    hits = [jnp.where(down_at == e, 1.0, 0.0).astype(bf16) for e in ids]
    lane_micro = (lax.broadcasted_iota(i32, (1, toks), 1) // tokens).astype(f32)
    within, passed = [], None
    for hit in hits:
        earlier = jnp.dot(hit, before, preferred_element_type=f32)
        if passed is not None:
            earlier = earlier + jnp.dot(passed, block, preferred_element_type=f32)
        place = jnp.sum(hit.astype(f32) * earlier, axis=0, keepdims=True)
        within.append(lane_micro * limit + place)
        passed = hit if passed is None else passed + hit
    tally = lax.dot_general(
        jnp.ones((8, toks), bf16), passed, (((1,), (1,)), ((), ())), preferred_element_type=f32
    )[0:1, :]
    rows = [ids[k].astype(f32) * cap + within[k] for k in range(picks)]
    rows += [across(weight_ref, k) for k in range(picks)] + [tally]
    line = lax.broadcasted_iota(i32, (8, toks), 0)
    own_meta = jnp.zeros((8, toks), f32)
    for i, row_of in enumerate(rows):
        own_meta = jnp.where(line == i, row_of, own_meta)
    meta_ref[...] = own_meta
    spread = jnp.zeros((8, pairs), f32)
    eight = lax.broadcasted_iota(i32, (8, toks), 0)
    for k in range(picks):
        put = jnp.where(
            lax.broadcasted_iota(i32, (toks, pairs), 1) == lax.broadcasted_iota(i32, (toks, pairs), 0) * picks + k, 1.0, 0.0
        ).astype(bf16)
        both = jnp.where(eight == 0, ids[k].astype(f32), within[k]).astype(bf16)
        spread = spread + jnp.dot(both, put, preferred_element_type=f32)
    pair_slot[...] = (spread[0:1, :] * cap + spread[1:2, :]).astype(i32)

    def fill(c):
        rows_here = hid_ref[:, :, :, c * step:(c + 1) * step].reshape(pairs, step)
        for i in range(2):
            sel = jnp.where(
                lax.broadcasted_iota(i32, (half, pairs), 0) + i * half == pair_slot[...], 1.0, 0.0
            ).astype(bf16)
            packed = jnp.dot(sel, rows_here, preferred_element_type=f32)
            hp[c, i] = packed.astype(bf16).reshape(NE, cap, step)

    fetches[2].wait()
    fill(FIRST)
    pl.semaphore_wait(barrier, len(partners))

    toward = [(g, (NY - GROUP_DY[g]) % NY, dxl) for g in range(NY) for dxl in (1, 0)]
    for g, dy, dxl in toward:
        if dxl or dy:
            send(meta_ref, meta.at[g * 2 + xlo], 0, s_meta.at[2], in_plane(dxl, dy)[2])
    keep(meta_ref, meta.at[xlo], s_meta.at[2])

    def first(g, dy, dxl):
        x2, y2, dev = in_plane(dxl, dy)
        piece = og_ref.at[:, :, pl.ds(pl.multiple_of((x2 * NY + y2) * cols, 128), cols)]
        if dxl or dy:
            send(piece, graw.at[g, 2, xlo], 2 if g else 1, s_first.at[g], dev)
        else:
            keep(piece, graw.at[g, 2, xlo], s_first.at[g])

    for which in toward:
        if which[0] < 2 or not which[2]:
            first(*which)

    def late(_):
        for which in toward:
            if which[0] >= 2 and which[2]:
                first(*which)

    def hid(c):
        for dz, dc in ZC:
            e, dev = zc(dz, dc)
            send(hp.at[c, :, e], hz.at[c, :, core, (2 - dz) % NZ], 3 if dz else 4, s_hz.at[c], dev)
        keep(hp.at[c, :, z * NC + core], hz.at[c, :, core, 2], s_hz.at[c])

    eye = jnp.where(
        lax.broadcasted_iota(jnp.int32, (256, 256), 0) == lax.broadcasted_iota(jnp.int32, (256, 256), 1), 1.0, 0.0
    ).astype(jnp.bfloat16)

    def turn(c):
        wait(hz.at[c], s_hz.at[c])
        for i in range(2):
            for f in range(0, step, 256):
                block = hz[c, i, :, :, :, f:f + 256].reshape(half, 256)
                turned = lax.dot_general(eye, block, (((1,), (1,)), ((), ())), preferred_element_type=jnp.float32)
                hzt[c, i, f:f + 256, :] = turned.astype(jnp.bfloat16)
        for dx in (1, 3, 2):
            h2, dev = along_x(dx)
            send(hzt.at[c, h2], ht.at[x, c], 5, s_hx.at[c], dev)
        keep(hzt.at[c, xhi], ht.at[x, c], s_hx.at[c])

    up, down = in_plane(0, 1)[2], in_plane(0, 3)[2]

    def row(c):
        own = ht.at[pl.ds(0, NX), c]
        wait(own, s_hx.at[c])
        send(own, ht.at[pl.ds(2 * NX, NX), c], 6, s_hy.at[0, c], up)
        send(own, ht.at[pl.ds(NX, NX), c], 6, s_hy.at[1, c], down)

    def relay(c):
        wait(ht.at[pl.ds(2 * NX, NX), c], s_hy.at[0, c])
        send(ht.at[pl.ds(2 * NX, 2), c], ht.at[pl.ds(3 * NX, 2), c], 7, s_hy.at[2, c], up)
        wait(ht.at[pl.ds(NX, NX), c], s_hy.at[1, c])
        send(ht.at[pl.ds(NX + 2, 2), c], ht.at[pl.ds(3 * NX + 2, 2), c], 7, s_hy.at[3, c], down)

    def routes(_):
        wait(meta, s_meta.at[2])
        for g in range(NY):
            near_meta[2, g] = jnp.concatenate([meta[2 * g, 0:4, :], meta[2 * g + 1, 0:4, :]], axis=0)
        total = meta[0, 4:5, :]
        for q in range(1, 2 * NY):
            total = total + meta[q, 4:5, :]
        cnt[...] = total
        for dz, at in ((1, 1), (7, 3), (2, 0), (6, 4)):
            send(near_meta.at[2], near_meta.at[at], 8, s_meta.at[at], zc(dz, 0)[1])

    plus, minus = zc(1, 0)[1], zc(7, 0)[1]

    def raw(g):
        wait(graw.at[g, 2], s_first.at[g])
        send(graw.at[g, 2], graw.at[g, 1], 9, s_raw.at[g, 1], plus)
        send(graw.at[g, 2], graw.at[g, 3], 9, s_raw.at[g, 3], minus)

    def far(g):
        wait(graw.at[g, 1], s_raw.at[g, 1])
        send(graw.at[g, 1], graw.at[g, 0], 9, s_raw.at[g, 0], plus)
        wait(graw.at[g, 3], s_raw.at[g, 3])
        send(graw.at[g, 3], graw.at[g, 4], 9, s_raw.at[g, 4], minus)

    chip_rows = 2 * NC * cap

    def slots_of(count, z1, h2, z2):
        r = lax.broadcasted_iota(jnp.int32, (count, toks), 0)
        gap = half - NC * cap
        near = r + jnp.where(r >= NC * cap, gap, 0) + z * (NC * cap)
        if count == chip_rows:
            return near.astype(jnp.float32)
        s = r - chip_rows
        beyond = s + jnp.where(s >= NC * cap, gap, 0) + z1 * (NC * cap)
        last = s - chip_rows + h2 * half + z2 * (NC * cap)
        return jnp.where(r < chip_rows, near, jnp.where(s < chip_rows, beyond, last)).astype(jnp.float32)

    def into_slots(g, sources, xls):
        @pl.loop(xls[0], xls[-1] + 1)
        def _(xl):
            for at in sources:
                if at == 0:
                    rows = slots_of(chip_rows * 5 // 2, lax.rem(z + 1, NZ), xhi, lax.rem(z + 2, NZ))
                elif at == NEAR - 1:
                    rows = slots_of(chip_rows * 5 // 2, lax.rem(z + 7, NZ), 1 - xhi, lax.rem(z + 6, NZ))
                else:
                    rows = slots_of(chip_rows, 0, 0, 0)
                info = jnp.where(xl == 0, near_meta[at, g, 0:4, :], near_meta[at, g, 4:8, :])
                first = rows == info[0:1, :]
                second = rows == info[1:2, :]
                weights = jnp.where(first, info[2:3, :], jnp.where(second, info[3:4, :], 0.0))
                weight = jnp.sum(weights, axis=1, keepdims=True)
                sel = jnp.where(first | second, 1.0, 0.0).astype(jnp.bfloat16)
                packed = jnp.dot(sel, graw[g, at, xl].reshape(toks, cols), preferred_element_type=jnp.float32) * weight
                packed = packed.astype(jnp.bfloat16)
                gnear[g, :, xl, at] = packed[:chip_rows].reshape(2 * NC, cap, cols)
                if at == 0 or at == NEAR - 1:
                    gfar[g, at // 4, :, xl] = packed[chip_rows:].reshape(3 * NC, cap, cols)

    def to_owners(g, first, count, xls):
        here, some = pl.ds(g * NX + xhi * 2 + xls[0], len(xls)), pl.ds(first, count)
        from_xl, sem = pl.ds(xls[0], len(xls)), s_gz.at[g + (xls[0] if g == NY - 1 else 0)]
        for dxh, dc in ((1, 0), (1, 1), (0, 1)):
            d, _, dev = owner(dxh, 0, dc)
            send(gnear.at[g, d, from_xl, some], gall.at[here, core, some], 11, sem, dev)
        keep(gnear.at[g, xhi * NC + core, from_xl, some], gall.at[here, core, some], sem)

    seen = set()

    def known(offsets):
        for at in offsets:
            if at not in seen:
                seen.add(at)
                wait(near_meta.at[at], s_meta.at[at])

    def near(g):
        known((1, 3))
        into_slots(g, (1, 2, 3), (0, 1))
        for xls in ((0, 1),) if g < NY - 1 else ((0,), (1,)):
            to_owners(g, 1, 3, xls)

    def pack(g, xl=0):
        xls = (xl,) if g == NY - 1 else (0, 1)
        known((0, 4))
        if xl == 0:
            wait(graw.at[g, 0], s_raw.at[g, 0])
            wait(graw.at[g, 4], s_raw.at[g, 4])
        into_slots(g, (0, 4), xls)
        here, from_xl = pl.ds(g * NX + xhi * 2 + xl, len(xls)), pl.ds(xl, len(xls))
        sem = s_gz.at[g + xl]
        for side, dz, at in ((0, 1, 7), (1, 7, 5)):
            for dxh in range(2):
                for dc in range(2):
                    d, _, dev = owner(dxh, dz, dc)
                    send(gfar.at[g, side, d, from_xl], gall.at[here, core, at], 10, sem, dev)
        for side, dz in ((0, 2), (1, 6)):
            for dc in range(2):
                _, c2, dev = owner(side, dz, dc)
                send(gfar.at[g, side, 2 * NC + c2, from_xl], gall.at[here, core, 6], 10, sem, dev)
        to_owners(g, 0, 1, xls)
        to_owners(g, 4, 1, xls)

    def count(part):
        if part == 0:
            me = z * NC + core
            for dz, dc in ZC:
                send(cnt, cnt_all.at[me], 12, s_cnt.at[0], zc(dz, dc)[1])
            keep(cnt, cnt_all.at[me], s_cnt.at[0])
            return
        if part == 2:
            send(cnt_x.at[0], cnt_x.at[1], 13, s_cnt.at[1], owner(1, 0, 0)[2])
            return
        wait(cnt_all, s_cnt.at[0])
        loads = cnt_all[0]
        for e in range(1, NE):
            loads = loads + cnt_all[e]
        cnt_x[0] = loads

    ready = set()

    def mul(g, c0, c1, xl=None):
        arrived = g if xl is None else g + xl
        if arrived not in ready:
            ready.add(arrived)
            wait(gall.at[pl.ds(g * NX, NX if xl is None else 2)], s_gz.at[arrived])
        if g == NY - 1 and xl == 0:
            for c in range(c0, c1):
                wait(ht.at[pl.ds(3 * NX, 2), c], s_hy.at[2, c])
                wait(ht.at[pl.ds(3 * NX + 2, 2), c], s_hy.at[3, c])

        @pl.loop(c0 // 2, c1 // 2)
        def _(pair):
            two = pl.ds(pair * 2, 2)
            at = pl.ds(pl.multiple_of(pair * 2 * step, 2 * step), 2 * step)
            part = None
            for xs in range(NX) if xl is None else (xl, xl + 2):
                q = g * NX + xs
                term = jnp.dot(ht[q, two].reshape(2 * step, half), gall[q].reshape(half, cols), preferred_element_type=jnp.float32)
                part = term if part is None else part + term
            if g == 0:
                acc[at, :] = part
            elif g < NY - 1 or xl == 0:
                acc[at, :] += part
            else:
                out_ref[0, at, :] = (acc[at, :] + part).astype(out_ref.dtype)

    steps = dict(fill=fill, late=late, near=near, count=count, hid=hid, routes=routes, raw=raw, turn=turn, far=far, row=row, relay=relay, pack=pack, mul=mul)
    for name, *which in ORDER:
        steps[name](*which)

    wait(cnt_x.at[1], s_cnt.at[1])
    load_ref[...] = ((cnt_x[0] + cnt_x[1]) / total_pairs)[0, :load_ref.shape[0]]

    sent = (
        meta.at[pl.ds(0, 7)], graw.at[0, 2, 0], graw.at[pl.ds(1, 3), 2], hz.at[:, :, :, pl.ds(0, 7)],
        hz.at[:, :, 0, 0], ht.at[pl.ds(0, 3)], ht.at[pl.ds(0, 2 * NX)], ht.at[pl.ds(0, NX)],
        near_meta.at[pl.ds(0, 4)], graw.at[:, pl.ds(0, 4)], gfar, gnear.at[:, pl.ds(0, 3)],
        cnt_all.at[pl.ds(0, NE - 1)], cnt_x.at[0],
    )
    for i, ref in enumerate(sent):
        wait(ref, s_send.at[i])


def body(hidden, out_grad, route_weight, expert_ids):
    micro, tokens, picks, ff = hidden.shape
    width = out_grad.shape[2]
    experts = lax.axis_size(EP)
    replicas = lax.axis_size(REP)
    cols = width // replicas
    limit = 2 * tokens * picks // experts
    cap = micro * limit
    toks = micro * tokens
    vmem = pl.BlockSpec(memory_space=pltpu.VMEM)
    bf16 = jnp.bfloat16
    dma = pltpu.SemaphoreType.DMA
    grad, load = pl.pallas_call(
        functools.partial(kernel, limit, float(micro * tokens * replicas * picks)),
        out_shape=(
            pltpu.VMEM((1, ff, cols), bf16),
            pltpu.VMEM((experts,), jnp.float32),
        ),
        in_specs=[pl.BlockSpec(memory_space=pl.ANY)] * 4,
        out_specs=(vmem, vmem),
        scratch_shapes=[
            pltpu.VMEM((micro, tokens, picks, ff), bf16),
            pltpu.VMEM((micro, picks, tokens), jnp.int32),
            pltpu.VMEM((micro, picks, tokens), jnp.float32),
            pltpu.VMEM((8, toks), jnp.float32),
            pltpu.VMEM((1, toks * picks), jnp.int32),
            pltpu.VMEM((NY, NEAR, 2, micro, tokens, cols), bf16),
            pltpu.VMEM((2 * NY, 8, toks), jnp.float32),
            pltpu.VMEM((NEAR, NY, 8, toks), jnp.float32),
            pltpu.VMEM((NY, 2 * NC, 2, NEAR, cap, cols), bf16),
            pltpu.VMEM((NY, 2, 3 * NC, 2, cap, cols), bf16),
            pltpu.VMEM((NQ, NC, NZ, cap, cols), bf16),
            pltpu.VMEM((CHUNKS, 2, NE, cap, ff // CHUNKS), bf16),
            pltpu.VMEM((CHUNKS, 2, NC, NZ, cap, ff // CHUNKS), bf16),
            pltpu.VMEM((CHUNKS, 2, ff // CHUNKS, NE * cap), bf16),
            pltpu.VMEM((NQ, CHUNKS, ff // CHUNKS, NE * cap), bf16),
            pltpu.VMEM((ff, cols), jnp.float32),
            pltpu.VMEM((1, toks), jnp.float32),
            pltpu.VMEM((NE, 1, toks), jnp.float32),
            pltpu.VMEM((2, 1, toks), jnp.float32),
            dma((14,)),
            dma((NEAR,)),
            dma((NY,)),
            dma((NY, NEAR)),
            dma((NY + 1,)),
            dma((CHUNKS,)),
            dma((CHUNKS,)),
            dma((4, CHUNKS)),
            dma((2,)),
            dma((3,)),
        ],
        compiler_params=pltpu.CompilerParams(
            collective_id=0, has_side_effects=True, vmem_limit_bytes=62_000_000 // 1024 * 1024
        ),
    )(hidden, expert_ids.transpose(0, 2, 1), route_weight.transpose(0, 2, 1), out_grad)
    return grad, load


def solution(mesh):
    finer = Mesh(mesh.devices.reshape(2, 4, 2, 8, 2), REP_EP)
    placed = (
        P(None, REP_EP, None, None),
        P(None, REP_EP, None),
        P(None, REP_EP, None),
        P(None, REP_EP, None),
    )
    return jax.shard_map(
        body, mesh=finer, in_specs=placed, out_specs=(P(EP, None, REP), P()), check_vma=False
    )
```

```python
import functools

import jax
import jax.numpy as jnp
from jax import lax
from jax.experimental import pallas as pl
from jax.experimental.pallas import tpu as pltpu
from jax.sharding import Mesh
from jax.sharding import PartitionSpec as P

REP_EP = ("rep_0", "rep_1", "ep_0", "ep_1", "ep_2")
EP = ("ep_0", "ep_1", "ep_2")
REP = ("rep_0", "rep_1")
MESH = pl.DeviceIdType.MESH
NX, NY, NZ, NC = 4, 4, 8, 2
NE = NZ * NC
NQ = NX * NY
NEAR = 5
CHUNKS = 8
ZC = [(1, 0), (7, 0), (1, 1), (7, 1), (2, 0), (6, 0), (2, 1), (6, 1), (3, 0), (5, 0), (3, 1), (5, 1), (4, 0), (4, 1), (0, 1)]
GROUP_DY = [0, 1, 3, 2]
FIRST = 0
ORDER = [
    ("hid", 0), ("fill", 6), ("hid", 6), ("fill", 5), ("fill", 3), ("fill", 1), ("raw", 0), ("fill", 4), ("turn", 0),
    ("hid", 1), ("turn", 6), ("late", 0), ("routes", 0), ("fill", 7), ("hid", 3), ("row", 0), ("far", 0), ("hid", 5),
    ("row", 6), ("raw", 1), ("near", 0), ("count", 0), ("turn", 1), ("hid", 7), ("turn", 3), ("relay", 0), ("raw", 2),
    ("fill", 2), ("raw", 3), ("pack", 0), ("hid", 4), ("relay", 6), ("row", 1), ("turn", 5), ("row", 3), ("hid", 2),
    ("far", 1), ("near", 1), ("relay", 1), ("far", 2), ("near", 2), ("row", 5), ("turn", 7), ("far", 3), ("near", 3),
    ("relay", 3), ("row", 7), ("turn", 4), ("turn", 2), ("relay", 5), ("row", 4), ("pack", 1), ("relay", 7),
    ("pack", 2), ("row", 2), ("pack", 3, 0), ("relay", 4), ("mul", 0, 0, 4), ("mul", 0, 4, 8), ("mul", 1, 4, 8),
    ("relay", 2), ("pack", 3, 1), ("mul", 1, 0, 4), ("count", 1), ("mul", 2, 4, 8), ("mul", 2, 0, 4),
    ("mul", 3, 4, 8, 0), ("mul", 3, 0, 4, 0), ("count", 2), ("mul", 3, 0, 4, 1), ("mul", 3, 4, 8, 1),
]


def kernel(limit, total_pairs, hid_hbm, ids_hbm, weight_hbm, og_ref, out_ref, load_ref,
           hid_ref, ids_ref, weight_ref, meta_ref, pair_slot, graw, meta, near_meta, gnear, gfar, gall, hp, hz, hzt, ht, acc, cnt, cnt_all, cnt_x,
           s_send, s_meta, s_first, s_raw, s_gz, s_hz, s_hx, s_hy, s_cnt, s_own):
    cap, step = hp.shape[3], hp.shape[4]
    cols = graw.shape[5]
    toks = graw.shape[3] * graw.shape[4]
    micro, tokens, picks = hid_ref.shape[:3]
    pairs = toks * picks
    half = NE * cap
    f32, bf16, i32 = jnp.float32, jnp.bfloat16, jnp.int32
    xlo, y = lax.axis_index("rep_0"), lax.axis_index("rep_1")
    xhi, z, core = lax.axis_index("ep_0"), lax.axis_index("ep_1"), lax.axis_index("ep_2")
    x = xhi * 2 + xlo

    def in_plane(dxl, dy):
        x2, y2 = lax.rem(xlo + dxl, 2), lax.rem(y + dy, NY)
        return x2, y2, {"rep_0": x2, "rep_1": y2}

    def along_x(dx):
        x2 = lax.rem(x + dx, NX)
        return x2 // 2, {"ep_0": x2 // 2, "rep_0": lax.rem(x2, 2)}

    def zc(dz, dc):
        z2, c2 = lax.rem(z + dz, NZ), lax.rem(core + dc, NC)
        return z2 * NC + c2, {"ep_1": z2, "ep_2": c2}

    def owner(dxh, dz, dc):
        h2, z2, c2 = lax.rem(xhi + dxh, 2), lax.rem(z + dz, NZ), lax.rem(core + dc, NC)
        return h2 * NC + c2, c2, {"ep_0": h2, "ep_1": z2, "ep_2": c2}

    def send(src, dst, send_sem, recv_sem, dev):
        pltpu.make_async_remote_copy(
            src_ref=src, dst_ref=dst, send_sem=s_send.at[send_sem], recv_sem=recv_sem, device_id=dev,
            device_id_type=MESH,
        ).start()

    def keep(src, dst, sem):
        pltpu.make_async_copy(src, dst, sem).start()

    def wait(ref, sem):
        pltpu.make_async_copy(ref, ref, sem).wait()

    barrier = pltpu.get_barrier_semaphore()
    partners = [in_plane(dxl, dy)[2] for dy in range(NY) for dxl in range(2) if dxl or dy]
    partners += [zc(dz, dc)[1] for dz, dc in ZC]
    partners += [{"ep_0": 1 - xhi, "rep_0": 1 - xlo}]
    partners += [owner(1, dz, dc)[2] for dz in (0, 1, 7, 2, 6) for dc in range(2)]
    for dev in partners:
        pl.semaphore_signal(barrier, inc=1, device_id=dev, device_id_type=MESH)

    fetches = [
        pltpu.make_async_copy(src, dst, s_own.at[i])
        for i, (src, dst) in enumerate(((ids_hbm, ids_ref), (weight_hbm, weight_ref), (hid_hbm, hid_ref)))
    ]
    for fetch in fetches:
        fetch.start()
    for fetch in fetches[:2]:
        fetch.wait()

    def across(ref, k):
        return jnp.concatenate([ref[m, k:k + 1, :] for m in range(micro)], axis=1)

    def square(rows):
        return lax.broadcasted_iota(i32, (rows, toks), 0), lax.broadcasted_iota(i32, (rows, toks), 1)

    down_at, along_at = square(toks)
    same = down_at // tokens == along_at // tokens
    block = jnp.where(same, 1.0, 0.0).astype(bf16)
    before = jnp.where(same & (down_at < along_at), 1.0, 0.0).astype(bf16)
    ids = [across(ids_ref, k) for k in range(picks)]
    hits = [jnp.where(down_at == e, 1.0, 0.0).astype(bf16) for e in ids]
    lane_micro = (lax.broadcasted_iota(i32, (1, toks), 1) // tokens).astype(f32)
    within, passed = [], None
    for hit in hits:
        earlier = jnp.dot(hit, before, preferred_element_type=f32)
        if passed is not None:
            earlier = earlier + jnp.dot(passed, block, preferred_element_type=f32)
        place = jnp.sum(hit.astype(f32) * earlier, axis=0, keepdims=True)
        within.append(lane_micro * limit + place)
        passed = hit if passed is None else passed + hit
    tally = lax.dot_general(
        jnp.ones((8, toks), bf16), passed, (((1,), (1,)), ((), ())), preferred_element_type=f32
    )[0:1, :]
    rows = [ids[k].astype(f32) * cap + within[k] for k in range(picks)]
    rows += [across(weight_ref, k) for k in range(picks)] + [tally]
    line = lax.broadcasted_iota(i32, (8, toks), 0)
    own_meta = jnp.zeros((8, toks), f32)
    for i, row_of in enumerate(rows):
        own_meta = jnp.where(line == i, row_of, own_meta)
    meta_ref[...] = own_meta
    spread = jnp.zeros((8, pairs), f32)
    eight = lax.broadcasted_iota(i32, (8, toks), 0)
    for k in range(picks):
        put = jnp.where(
            lax.broadcasted_iota(i32, (toks, pairs), 1) == lax.broadcasted_iota(i32, (toks, pairs), 0) * picks + k, 1.0, 0.0
        ).astype(bf16)
        both = jnp.where(eight == 0, ids[k].astype(f32), within[k]).astype(bf16)
        spread = spread + jnp.dot(both, put, preferred_element_type=f32)
    pair_slot[...] = (spread[0:1, :] * cap + spread[1:2, :]).astype(i32)

    def fill(c):
        rows_here = hid_ref[:, :, :, c * step:(c + 1) * step].reshape(pairs, step)
        for i in range(2):
            sel = jnp.where(
                lax.broadcasted_iota(i32, (half, pairs), 0) + i * half == pair_slot[...], 1.0, 0.0
            ).astype(bf16)
            packed = jnp.dot(sel, rows_here, preferred_element_type=f32)
            hp[c, i] = packed.astype(bf16).reshape(NE, cap, step)

    fetches[2].wait()
    fill(FIRST)
    pl.semaphore_wait(barrier, len(partners))

    toward = [(g, (NY - GROUP_DY[g]) % NY, dxl) for g in range(NY) for dxl in (1, 0)]
    for g, dy, dxl in toward:
        if dxl or dy:
            send(meta_ref, meta.at[g * 2 + xlo], 0, s_meta.at[2], in_plane(dxl, dy)[2])
    keep(meta_ref, meta.at[xlo], s_meta.at[2])

    def first(g, dy, dxl):
        x2, y2, dev = in_plane(dxl, dy)
        piece = og_ref.at[:, :, pl.ds(pl.multiple_of((x2 * NY + y2) * cols, 128), cols)]
        if dxl or dy:
            send(piece, graw.at[g, 2, xlo], 2 if g else 1, s_first.at[g], dev)
        else:
            keep(piece, graw.at[g, 2, xlo], s_first.at[g])

    for which in toward:
        if which[0] < 2 or not which[2]:
            first(*which)

    def late(_):
        for which in toward:
            if which[0] >= 2 and which[2]:
                first(*which)

    def hid(c):
        for dz, dc in ZC:
            e, dev = zc(dz, dc)
            send(hp.at[c, :, e], hz.at[c, :, core, (2 - dz) % NZ], 3 if dz else 4, s_hz.at[c], dev)
        keep(hp.at[c, :, z * NC + core], hz.at[c, :, core, 2], s_hz.at[c])

    eye = jnp.where(
        lax.broadcasted_iota(jnp.int32, (256, 256), 0) == lax.broadcasted_iota(jnp.int32, (256, 256), 1), 1.0, 0.0
    ).astype(jnp.bfloat16)

    def turn(c):
        wait(hz.at[c], s_hz.at[c])
        for i in range(2):
            for f in range(0, step, 256):
                block = hz[c, i, :, :, :, f:f + 256].reshape(half, 256)
                turned = lax.dot_general(eye, block, (((1,), (1,)), ((), ())), preferred_element_type=jnp.float32)
                hzt[c, i, f:f + 256, :] = turned.astype(jnp.bfloat16)
        for dx in (1, 3, 2):
            h2, dev = along_x(dx)
            send(hzt.at[c, h2], ht.at[x, c], 5, s_hx.at[c], dev)
        keep(hzt.at[c, xhi], ht.at[x, c], s_hx.at[c])

    up, down = in_plane(0, 1)[2], in_plane(0, 3)[2]

    def row(c):
        own = ht.at[pl.ds(0, NX), c]
        wait(own, s_hx.at[c])
        send(own, ht.at[pl.ds(2 * NX, NX), c], 6, s_hy.at[0, c], up)
        send(own, ht.at[pl.ds(NX, NX), c], 6, s_hy.at[1, c], down)

    def relay(c):
        wait(ht.at[pl.ds(2 * NX, NX), c], s_hy.at[0, c])
        send(ht.at[pl.ds(2 * NX, 2), c], ht.at[pl.ds(3 * NX, 2), c], 7, s_hy.at[2, c], up)
        wait(ht.at[pl.ds(NX, NX), c], s_hy.at[1, c])
        send(ht.at[pl.ds(NX + 2, 2), c], ht.at[pl.ds(3 * NX + 2, 2), c], 7, s_hy.at[3, c], down)

    def routes(_):
        wait(meta, s_meta.at[2])
        for g in range(NY):
            near_meta[2, g] = jnp.concatenate([meta[2 * g, 0:4, :], meta[2 * g + 1, 0:4, :]], axis=0)
        total = meta[0, 4:5, :]
        for q in range(1, 2 * NY):
            total = total + meta[q, 4:5, :]
        cnt[...] = total
        for dz, at in ((1, 1), (7, 3), (2, 0), (6, 4)):
            send(near_meta.at[2], near_meta.at[at], 8, s_meta.at[at], zc(dz, 0)[1])

    plus, minus = zc(1, 0)[1], zc(7, 0)[1]

    def raw(g):
        wait(graw.at[g, 2], s_first.at[g])
        send(graw.at[g, 2], graw.at[g, 1], 9, s_raw.at[g, 1], plus)
        send(graw.at[g, 2], graw.at[g, 3], 9, s_raw.at[g, 3], minus)

    def far(g):
        wait(graw.at[g, 1], s_raw.at[g, 1])
        send(graw.at[g, 1], graw.at[g, 0], 9, s_raw.at[g, 0], plus)
        wait(graw.at[g, 3], s_raw.at[g, 3])
        send(graw.at[g, 3], graw.at[g, 4], 9, s_raw.at[g, 4], minus)

    chip_rows = 2 * NC * cap

    def slots_of(count, z1, h2, z2):
        r = lax.broadcasted_iota(jnp.int32, (count, toks), 0)
        gap = half - NC * cap
        near = r + jnp.where(r >= NC * cap, gap, 0) + z * (NC * cap)
        if count == chip_rows:
            return near.astype(jnp.float32)
        s = r - chip_rows
        beyond = s + jnp.where(s >= NC * cap, gap, 0) + z1 * (NC * cap)
        last = s - chip_rows + h2 * half + z2 * (NC * cap)
        return jnp.where(r < chip_rows, near, jnp.where(s < chip_rows, beyond, last)).astype(jnp.float32)

    def into_slots(g, sources, xls):
        @pl.loop(xls[0], xls[-1] + 1)
        def _(xl):
            for at in sources:
                if at == 0:
                    rows = slots_of(chip_rows * 5 // 2, lax.rem(z + 1, NZ), xhi, lax.rem(z + 2, NZ))
                elif at == NEAR - 1:
                    rows = slots_of(chip_rows * 5 // 2, lax.rem(z + 7, NZ), 1 - xhi, lax.rem(z + 6, NZ))
                else:
                    rows = slots_of(chip_rows, 0, 0, 0)
                info = jnp.where(xl == 0, near_meta[at, g, 0:4, :], near_meta[at, g, 4:8, :])
                first = rows == info[0:1, :]
                second = rows == info[1:2, :]
                weights = jnp.where(first, info[2:3, :], jnp.where(second, info[3:4, :], 0.0))
                weight = jnp.sum(weights, axis=1, keepdims=True)
                sel = jnp.where(first | second, 1.0, 0.0).astype(jnp.bfloat16)
                packed = jnp.dot(sel, graw[g, at, xl].reshape(toks, cols), preferred_element_type=jnp.float32) * weight
                packed = packed.astype(jnp.bfloat16)
                gnear[g, :, xl, at] = packed[:chip_rows].reshape(2 * NC, cap, cols)
                if at == 0 or at == NEAR - 1:
                    gfar[g, at // 4, :, xl] = packed[chip_rows:].reshape(3 * NC, cap, cols)

    def to_owners(g, first, count, xls):
        here, some = pl.ds(g * NX + xhi * 2 + xls[0], len(xls)), pl.ds(first, count)
        from_xl, sem = pl.ds(xls[0], len(xls)), s_gz.at[g + (xls[0] if g == NY - 1 else 0)]
        for dxh, dc in ((1, 0), (1, 1), (0, 1)):
            d, _, dev = owner(dxh, 0, dc)
            send(gnear.at[g, d, from_xl, some], gall.at[here, core, some], 11, sem, dev)
        keep(gnear.at[g, xhi * NC + core, from_xl, some], gall.at[here, core, some], sem)

    seen = set()

    def known(offsets):
        for at in offsets:
            if at not in seen:
                seen.add(at)
                wait(near_meta.at[at], s_meta.at[at])

    def near(g):
        known((1, 3))
        into_slots(g, (1, 2, 3), (0, 1))
        for xls in ((0, 1),) if g < NY - 1 else ((0,), (1,)):
            to_owners(g, 1, 3, xls)

    def pack(g, xl=0):
        xls = (xl,) if g == NY - 1 else (0, 1)
        known((0, 4))
        if xl == 0:
            wait(graw.at[g, 0], s_raw.at[g, 0])
            wait(graw.at[g, 4], s_raw.at[g, 4])
        into_slots(g, (0, 4), xls)
        here, from_xl = pl.ds(g * NX + xhi * 2 + xl, len(xls)), pl.ds(xl, len(xls))
        sem = s_gz.at[g + xl]
        for side, dz, at in ((0, 1, 7), (1, 7, 5)):
            for dxh in range(2):
                for dc in range(2):
                    d, _, dev = owner(dxh, dz, dc)
                    send(gfar.at[g, side, d, from_xl], gall.at[here, core, at], 10, sem, dev)
        for side, dz in ((0, 2), (1, 6)):
            for dc in range(2):
                _, c2, dev = owner(side, dz, dc)
                send(gfar.at[g, side, 2 * NC + c2, from_xl], gall.at[here, core, 6], 10, sem, dev)
        to_owners(g, 0, 1, xls)
        to_owners(g, 4, 1, xls)

    def count(part):
        if part == 0:
            me = z * NC + core
            for dz, dc in ZC:
                send(cnt, cnt_all.at[me], 12, s_cnt.at[0], zc(dz, dc)[1])
            keep(cnt, cnt_all.at[me], s_cnt.at[0])
            return
        if part == 2:
            send(cnt_x.at[0], cnt_x.at[1], 13, s_cnt.at[1], owner(1, 0, 0)[2])
            return
        wait(cnt_all, s_cnt.at[0])
        loads = cnt_all[0]
        for e in range(1, NE):
            loads = loads + cnt_all[e]
        cnt_x[0] = loads

    ready = set()

    def mul(g, c0, c1, xl=None):
        arrived = g if xl is None else g + xl
        if arrived not in ready:
            ready.add(arrived)
            wait(gall.at[pl.ds(g * NX, NX if xl is None else 2)], s_gz.at[arrived])
        if g == NY - 1 and xl == 0:
            for c in range(c0, c1):
                wait(ht.at[pl.ds(3 * NX, 2), c], s_hy.at[2, c])
                wait(ht.at[pl.ds(3 * NX + 2, 2), c], s_hy.at[3, c])

        @pl.loop(c0 // 4, c1 // 4)
        def _(pair):
            two = pl.ds(pair * 4, 4)
            at = pl.ds(pl.multiple_of(pair * 4 * step, 4 * step), 4 * step)
            part = None
            for xs in range(NX) if xl is None else (xl, xl + 2):
                q = g * NX + xs
                term = jnp.dot(ht[q, two].reshape(4 * step, half), gall[q].reshape(half, cols), preferred_element_type=jnp.float32)
                part = term if part is None else part + term
            if g == 0:
                acc[at, :] = part
            elif g < NY - 1 or xl == 0:
                acc[at, :] += part
            else:
                out_ref[0, at, :] = (acc[at, :] + part).astype(out_ref.dtype)

    steps = dict(fill=fill, late=late, near=near, count=count, hid=hid, routes=routes, raw=raw, turn=turn, far=far, row=row, relay=relay, pack=pack, mul=mul)
    for name, *which in ORDER:
        steps[name](*which)

    wait(cnt_x.at[1], s_cnt.at[1])
    load_ref[...] = ((cnt_x[0] + cnt_x[1]) / total_pairs)[0, :load_ref.shape[0]]

    sent = (
        meta.at[pl.ds(0, 7)], graw.at[0, 2, 0], graw.at[pl.ds(1, 3), 2], hz.at[:, :, :, pl.ds(0, 7)],
        hz.at[:, :, 0, 0], ht.at[pl.ds(0, 3)], ht.at[pl.ds(0, 2 * NX)], ht.at[pl.ds(0, NX)],
        near_meta.at[pl.ds(0, 4)], graw.at[:, pl.ds(0, 4)], gfar, gnear.at[:, pl.ds(0, 3)],
        cnt_all.at[pl.ds(0, NE - 1)], cnt_x.at[0],
    )
    for i, ref in enumerate(sent):
        wait(ref, s_send.at[i])


def body(hidden, out_grad, route_weight, expert_ids):
    micro, tokens, picks, ff = hidden.shape
    width = out_grad.shape[2]
    experts = lax.axis_size(EP)
    replicas = lax.axis_size(REP)
    cols = width // replicas
    limit = 2 * tokens * picks // experts
    cap = micro * limit
    toks = micro * tokens
    vmem = pl.BlockSpec(memory_space=pltpu.VMEM)
    bf16 = jnp.bfloat16
    dma = pltpu.SemaphoreType.DMA
    grad, load = pl.pallas_call(
        functools.partial(kernel, limit, float(micro * tokens * replicas * picks)),
        out_shape=(
            pltpu.VMEM((1, ff, cols), bf16),
            pltpu.VMEM((experts,), jnp.float32),
        ),
        in_specs=[pl.BlockSpec(memory_space=pl.ANY)] * 4,
        out_specs=(vmem, vmem),
        scratch_shapes=[
            pltpu.VMEM((micro, tokens, picks, ff), bf16),
            pltpu.VMEM((micro, picks, tokens), jnp.int32),
            pltpu.VMEM((micro, picks, tokens), jnp.float32),
            pltpu.VMEM((8, toks), jnp.float32),
            pltpu.VMEM((1, toks * picks), jnp.int32),
            pltpu.VMEM((NY, NEAR, 2, micro, tokens, cols), bf16),
            pltpu.VMEM((2 * NY, 8, toks), jnp.float32),
            pltpu.VMEM((NEAR, NY, 8, toks), jnp.float32),
            pltpu.VMEM((NY, 2 * NC, 2, NEAR, cap, cols), bf16),
            pltpu.VMEM((NY, 2, 3 * NC, 2, cap, cols), bf16),
            pltpu.VMEM((NQ, NC, NZ, cap, cols), bf16),
            pltpu.VMEM((CHUNKS, 2, NE, cap, ff // CHUNKS), bf16),
            pltpu.VMEM((CHUNKS, 2, NC, NZ, cap, ff // CHUNKS), bf16),
            pltpu.VMEM((CHUNKS, 2, ff // CHUNKS, NE * cap), bf16),
            pltpu.VMEM((NQ, CHUNKS, ff // CHUNKS, NE * cap), bf16),
            pltpu.VMEM((ff, cols), jnp.float32),
            pltpu.VMEM((1, toks), jnp.float32),
            pltpu.VMEM((NE, 1, toks), jnp.float32),
            pltpu.VMEM((2, 1, toks), jnp.float32),
            dma((14,)),
            dma((NEAR,)),
            dma((NY,)),
            dma((NY, NEAR)),
            dma((NY + 1,)),
            dma((CHUNKS,)),
            dma((CHUNKS,)),
            dma((4, CHUNKS)),
            dma((2,)),
            dma((3,)),
        ],
        compiler_params=pltpu.CompilerParams(
            collective_id=0, has_side_effects=True, vmem_limit_bytes=62_000_000 // 1024 * 1024
        ),
    )(hidden, expert_ids.transpose(0, 2, 1), route_weight.transpose(0, 2, 1), out_grad)
    return grad, load


def solution(mesh):
    finer = Mesh(mesh.devices.reshape(2, 4, 2, 8, 2), REP_EP)
    placed = (
        P(None, REP_EP, None, None),
        P(None, REP_EP, None),
        P(None, REP_EP, None),
        P(None, REP_EP, None),
    )
    return jax.shard_map(
        body, mesh=finer, in_specs=placed, out_specs=(P(EP, None, REP), P()), check_vma=False
    )
```

```python
import functools

import jax
import jax.numpy as jnp
from jax import lax
from jax.experimental import pallas as pl
from jax.experimental.pallas import tpu as pltpu
from jax.sharding import Mesh
from jax.sharding import PartitionSpec as P

REP_EP = ("rep_0", "rep_1", "ep_0", "ep_1", "ep_2")
EP = ("ep_0", "ep_1", "ep_2")
REP = ("rep_0", "rep_1")
MESH = pl.DeviceIdType.MESH
NX, NY, NZ, NC = 4, 4, 8, 2
NE = NZ * NC
NQ = NX * NY
NEAR = 5
CHUNKS = 8
ZC = [(1, 0), (7, 0), (1, 1), (7, 1), (2, 0), (6, 0), (2, 1), (6, 1), (3, 0), (5, 0), (3, 1), (5, 1), (4, 0), (4, 1), (0, 1)]
GROUP_DY = [0, 1, 3, 2]
FIRST = 0
ORDER = [
    ("hid", 0), ("fill", 6), ("hid", 6), ("fill", 5), ("fill", 3), ("fill", 1), ("raw", 0), ("fill", 4), ("turn", 0),
    ("hid", 1), ("turn", 6), ("late", 0), ("routes", 0), ("fill", 7), ("hid", 3), ("row", 0), ("far", 0), ("hid", 5),
    ("row", 6), ("raw", 1), ("near", 0), ("count", 0), ("turn", 1), ("hid", 7), ("turn", 3), ("relay", 0), ("raw", 2),
    ("fill", 2), ("raw", 3), ("pack", 0), ("hid", 4), ("relay", 6), ("row", 1), ("turn", 5), ("row", 3), ("hid", 2),
    ("far", 1), ("near", 1), ("relay", 1), ("far", 2), ("near", 2), ("row", 5), ("turn", 7), ("far", 3), ("near", 3),
    ("relay", 3), ("row", 7), ("turn", 4), ("turn", 2), ("relay", 5), ("row", 4), ("pack", 1), ("relay", 7),
    ("pack", 2), ("row", 2), ("pack", 3, 0), ("relay", 4), ("mul", 0, 0, 4), ("mul", 0, 4, 8), ("mul", 1, 4, 8),
    ("relay", 2), ("pack", 3, 1), ("mul", 1, 0, 4), ("count", 1), ("mul", 2, 4, 8), ("mul", 2, 0, 4),
    ("mul", 3, 4, 8, 0), ("mul", 3, 0, 4, 0), ("count", 2), ("mul", 3, 0, 4, 1), ("mul", 3, 4, 8, 1),
]


def kernel(limit, total_pairs, hid_hbm, ids_hbm, weight_hbm, og_ref, out_ref, load_ref,
           hid_ref, ids_ref, weight_ref, meta_ref, pair_slot, graw, meta, near_meta, gnear, gfar, gall, hp, hz, hzt, ht, acc, cnt, cnt_all, cnt_x,
           s_send, s_meta, s_first, s_raw, s_gz, s_hz, s_hx, s_hy, s_cnt, s_own):
    cap, step = hp.shape[3], hp.shape[4]
    cols = graw.shape[5]
    toks = graw.shape[3] * graw.shape[4]
    micro, tokens, picks = hid_ref.shape[:3]
    pairs = toks * picks
    half = NE * cap
    f32, bf16, i32 = jnp.float32, jnp.bfloat16, jnp.int32
    xlo, y = lax.axis_index("rep_0"), lax.axis_index("rep_1")
    xhi, z, core = lax.axis_index("ep_0"), lax.axis_index("ep_1"), lax.axis_index("ep_2")
    x = xhi * 2 + xlo

    def in_plane(dxl, dy):
        x2, y2 = lax.rem(xlo + dxl, 2), lax.rem(y + dy, NY)
        return x2, y2, {"rep_0": x2, "rep_1": y2}

    def along_x(dx):
        x2 = lax.rem(x + dx, NX)
        return x2 // 2, {"ep_0": x2 // 2, "rep_0": lax.rem(x2, 2)}

    def zc(dz, dc):
        z2, c2 = lax.rem(z + dz, NZ), lax.rem(core + dc, NC)
        return z2 * NC + c2, {"ep_1": z2, "ep_2": c2}

    def owner(dxh, dz, dc):
        h2, z2, c2 = lax.rem(xhi + dxh, 2), lax.rem(z + dz, NZ), lax.rem(core + dc, NC)
        return h2 * NC + c2, c2, {"ep_0": h2, "ep_1": z2, "ep_2": c2}

    def send(src, dst, send_sem, recv_sem, dev):
        pltpu.make_async_remote_copy(
            src_ref=src, dst_ref=dst, send_sem=s_send.at[send_sem], recv_sem=recv_sem, device_id=dev,
            device_id_type=MESH,
        ).start()

    def keep(src, dst, sem):
        pltpu.make_async_copy(src, dst, sem).start()

    def wait(ref, sem):
        pltpu.make_async_copy(ref, ref, sem).wait()

    barrier = pltpu.get_barrier_semaphore()
    partners = [in_plane(dxl, dy)[2] for dy in range(NY) for dxl in range(2) if dxl or dy]
    partners += [zc(dz, dc)[1] for dz, dc in ZC]
    partners += [{"ep_0": 1 - xhi, "rep_0": 1 - xlo}]
    partners += [owner(1, dz, dc)[2] for dz in (0, 1, 7, 2, 6) for dc in range(2)]
    for dev in partners:
        pl.semaphore_signal(barrier, inc=1, device_id=dev, device_id_type=MESH)

    fetches = [
        pltpu.make_async_copy(src, dst, s_own.at[i])
        for i, (src, dst) in enumerate(((ids_hbm, ids_ref), (weight_hbm, weight_ref), (hid_hbm, hid_ref)))
    ]
    for fetch in fetches:
        fetch.start()
    for fetch in fetches[:2]:
        fetch.wait()

    def across(ref, k):
        return jnp.concatenate([ref[m, k:k + 1, :] for m in range(micro)], axis=1)

    def square(rows):
        return lax.broadcasted_iota(i32, (rows, toks), 0), lax.broadcasted_iota(i32, (rows, toks), 1)

    down_at, along_at = square(toks)
    same = down_at // tokens == along_at // tokens
    block = jnp.where(same, 1.0, 0.0).astype(bf16)
    before = jnp.where(same & (down_at < along_at), 1.0, 0.0).astype(bf16)
    ids = [across(ids_ref, k) for k in range(picks)]
    hits = [jnp.where(down_at == e, 1.0, 0.0).astype(bf16) for e in ids]
    lane_micro = (lax.broadcasted_iota(i32, (1, toks), 1) // tokens).astype(f32)
    within, passed = [], None
    for hit in hits:
        earlier = jnp.dot(hit, before, preferred_element_type=f32)
        if passed is not None:
            earlier = earlier + jnp.dot(passed, block, preferred_element_type=f32)
        place = jnp.sum(hit.astype(f32) * earlier, axis=0, keepdims=True)
        within.append(lane_micro * limit + place)
        passed = hit if passed is None else passed + hit
    tally = lax.dot_general(
        jnp.ones((8, toks), bf16), passed, (((1,), (1,)), ((), ())), preferred_element_type=f32
    )[0:1, :]
    rows = [ids[k].astype(f32) * cap + within[k] for k in range(picks)]
    rows += [across(weight_ref, k) for k in range(picks)] + [tally]
    line = lax.broadcasted_iota(i32, (8, toks), 0)
    own_meta = jnp.zeros((8, toks), f32)
    for i, row_of in enumerate(rows):
        own_meta = jnp.where(line == i, row_of, own_meta)
    meta_ref[...] = own_meta
    spread = jnp.zeros((8, pairs), f32)
    eight = lax.broadcasted_iota(i32, (8, toks), 0)
    for k in range(picks):
        put = jnp.where(
            lax.broadcasted_iota(i32, (toks, pairs), 1) == lax.broadcasted_iota(i32, (toks, pairs), 0) * picks + k, 1.0, 0.0
        ).astype(bf16)
        both = jnp.where(eight == 0, ids[k].astype(f32), within[k]).astype(bf16)
        spread = spread + jnp.dot(both, put, preferred_element_type=f32)
    pair_slot[...] = (spread[0:1, :] * cap + spread[1:2, :]).astype(i32)

    def fill(c):
        rows_here = hid_ref[:, :, :, c * step:(c + 1) * step].reshape(pairs, step)
        for i in range(2):
            sel = jnp.where(
                lax.broadcasted_iota(i32, (half, pairs), 0) + i * half == pair_slot[...], 1.0, 0.0
            ).astype(bf16)
            packed = jnp.dot(sel, rows_here, preferred_element_type=f32)
            hp[c, i] = packed.astype(bf16).reshape(NE, cap, step)

    fetches[2].wait()
    fill(FIRST)
    pl.semaphore_wait(barrier, len(partners))

    toward = [(g, (NY - GROUP_DY[g]) % NY, dxl) for g in range(NY) for dxl in (1, 0)]
    for g, dy, dxl in toward:
        if dxl or dy:
            send(meta_ref, meta.at[g * 2 + xlo], 0, s_meta.at[2], in_plane(dxl, dy)[2])
    keep(meta_ref, meta.at[xlo], s_meta.at[2])

    def first(g, dy, dxl):
        x2, y2, dev = in_plane(dxl, dy)
        piece = og_ref.at[:, :, pl.ds(pl.multiple_of((x2 * NY + y2) * cols, 128), cols)]
        if dxl or dy:
            send(piece, graw.at[g, 2, xlo], 2 if g else 1, s_first.at[g], dev)
        else:
            keep(piece, graw.at[g, 2, xlo], s_first.at[g])

    for which in toward:
        if which[0] < 2 or not which[2]:
            first(*which)

    def late(_):
        for which in toward:
            if which[0] >= 2 and which[2]:
                first(*which)

    def hid(c):
        for dz, dc in ZC:
            e, dev = zc(dz, dc)
            send(hp.at[c, :, e], hz.at[c, :, core, (2 - dz) % NZ], 3 if dz else 4, s_hz.at[c], dev)
        keep(hp.at[c, :, z * NC + core], hz.at[c, :, core, 2], s_hz.at[c])

    eye = jnp.where(
        lax.broadcasted_iota(jnp.int32, (256, 256), 0) == lax.broadcasted_iota(jnp.int32, (256, 256), 1), 1.0, 0.0
    ).astype(jnp.bfloat16)

    def turn(c):
        wait(hz.at[c], s_hz.at[c])
        for i in range(2):
            for f in range(0, step, 256):
                block = hz[c, i, :, :, :, f:f + 256].reshape(half, 256)
                turned = lax.dot_general(eye, block, (((1,), (1,)), ((), ())), preferred_element_type=jnp.float32)
                hzt[c, i, f:f + 256, :] = turned.astype(jnp.bfloat16)
        for dx in (1, 3, 2):
            h2, dev = along_x(dx)
            send(hzt.at[c, h2], ht.at[x, c], 5, s_hx.at[c], dev)
        keep(hzt.at[c, xhi], ht.at[x, c], s_hx.at[c])

    up, down = in_plane(0, 1)[2], in_plane(0, 3)[2]

    def row(c):
        own = ht.at[pl.ds(0, NX), c]
        wait(own, s_hx.at[c])
        send(own, ht.at[pl.ds(2 * NX, NX), c], 6, s_hy.at[0, c], up)
        send(own, ht.at[pl.ds(NX, NX), c], 6, s_hy.at[1, c], down)

    def relay(c):
        wait(ht.at[pl.ds(2 * NX, NX), c], s_hy.at[0, c])
        send(ht.at[pl.ds(2 * NX, 2), c], ht.at[pl.ds(3 * NX, 2), c], 7, s_hy.at[2, c], up)
        wait(ht.at[pl.ds(NX, NX), c], s_hy.at[1, c])
        send(ht.at[pl.ds(NX + 2, 2), c], ht.at[pl.ds(3 * NX + 2, 2), c], 7, s_hy.at[3, c], down)

    def routes(_):
        wait(meta, s_meta.at[2])
        for g in range(NY):
            near_meta[2, g] = jnp.concatenate([meta[2 * g, 0:4, :], meta[2 * g + 1, 0:4, :]], axis=0)
        total = meta[0, 4:5, :]
        for q in range(1, 2 * NY):
            total = total + meta[q, 4:5, :]
        cnt[...] = total
        for dz, at in ((1, 1), (7, 3), (2, 0), (6, 4)):
            send(near_meta.at[2], near_meta.at[at], 8, s_meta.at[at], zc(dz, 0)[1])

    plus, minus = zc(1, 0)[1], zc(7, 0)[1]

    def raw(g):
        wait(graw.at[g, 2], s_first.at[g])
        send(graw.at[g, 2], graw.at[g, 1], 9, s_raw.at[g, 1], plus)
        send(graw.at[g, 2], graw.at[g, 3], 9, s_raw.at[g, 3], minus)

    def far(g):
        wait(graw.at[g, 1], s_raw.at[g, 1])
        send(graw.at[g, 1], graw.at[g, 0], 9, s_raw.at[g, 0], plus)
        wait(graw.at[g, 3], s_raw.at[g, 3])
        send(graw.at[g, 3], graw.at[g, 4], 9, s_raw.at[g, 4], minus)

    chip_rows = 2 * NC * cap

    def slots_of(count, z1, h2, z2):
        r = lax.broadcasted_iota(jnp.int32, (count, toks), 0)
        gap = half - NC * cap
        near = r + jnp.where(r >= NC * cap, gap, 0) + z * (NC * cap)
        if count == chip_rows:
            return near.astype(jnp.float32)
        s = r - chip_rows
        beyond = s + jnp.where(s >= NC * cap, gap, 0) + z1 * (NC * cap)
        last = s - chip_rows + h2 * half + z2 * (NC * cap)
        return jnp.where(r < chip_rows, near, jnp.where(s < chip_rows, beyond, last)).astype(jnp.float32)

    def into_slots(g, sources, xls):
        @pl.loop(xls[0], xls[-1] + 1)
        def _(xl):
            for at in sources:
                if at == 0:
                    rows = slots_of(chip_rows * 5 // 2, lax.rem(z + 1, NZ), xhi, lax.rem(z + 2, NZ))
                elif at == NEAR - 1:
                    rows = slots_of(chip_rows * 5 // 2, lax.rem(z + 7, NZ), 1 - xhi, lax.rem(z + 6, NZ))
                else:
                    rows = slots_of(chip_rows, 0, 0, 0)
                info = jnp.where(xl == 0, near_meta[at, g, 0:4, :], near_meta[at, g, 4:8, :])
                first = rows == info[0:1, :]
                second = rows == info[1:2, :]
                weights = jnp.where(first, info[2:3, :], jnp.where(second, info[3:4, :], 0.0))
                weight = jnp.sum(weights, axis=1, keepdims=True)
                sel = jnp.where(first | second, 1.0, 0.0).astype(jnp.bfloat16)
                packed = jnp.dot(sel, graw[g, at, xl].reshape(toks, cols), preferred_element_type=jnp.float32) * weight
                packed = packed.astype(jnp.bfloat16)
                gnear[g, :, xl, at] = packed[:chip_rows].reshape(2 * NC, cap, cols)
                if at == 0 or at == NEAR - 1:
                    gfar[g, at // 4, :, xl] = packed[chip_rows:].reshape(3 * NC, cap, cols)

    def to_owners(g, first, count, xls):
        here, some = pl.ds(g * NX + xhi * 2 + xls[0], len(xls)), pl.ds(first, count)
        from_xl, sem = pl.ds(xls[0], len(xls)), s_gz.at[g + (xls[0] if g == NY - 1 else 0)]
        for dxh, dc in ((1, 0), (1, 1), (0, 1)):
            d, _, dev = owner(dxh, 0, dc)
            send(gnear.at[g, d, from_xl, some], gall.at[here, core, some], 11, sem, dev)
        keep(gnear.at[g, xhi * NC + core, from_xl, some], gall.at[here, core, some], sem)

    seen = set()

    def known(offsets):
        for at in offsets:
            if at not in seen:
                seen.add(at)
                wait(near_meta.at[at], s_meta.at[at])

    def near(g):
        known((1, 3))
        into_slots(g, (1, 2, 3), (0, 1))
        for xls in ((0, 1),) if g < NY - 1 else ((0,), (1,)):
            to_owners(g, 1, 3, xls)

    def pack(g, xl=0):
        xls = (xl,) if g == NY - 1 else (0, 1)
        known((0, 4))
        if xl == 0:
            wait(graw.at[g, 0], s_raw.at[g, 0])
            wait(graw.at[g, 4], s_raw.at[g, 4])
        into_slots(g, (0, 4), xls)
        here, from_xl = pl.ds(g * NX + xhi * 2 + xl, len(xls)), pl.ds(xl, len(xls))
        sem = s_gz.at[g + xl]
        for dc in range(2):
            for side, dz in ((0, 2), (1, 6)):
                _, c2, dev = owner(side, dz, dc)
                send(gfar.at[g, side, 2 * NC + c2, from_xl], gall.at[here, core, 6], 10, sem, dev)
        for dxh in (1, 0):
            for dc in range(2):
                for side, dz, at in ((0, 1, 7), (1, 7, 5)):
                    d, _, dev = owner(dxh, dz, dc)
                    send(gfar.at[g, side, d, from_xl], gall.at[here, core, at], 10, sem, dev)
        to_owners(g, 0, 1, xls)
        to_owners(g, 4, 1, xls)

    def count(part):
        if part == 0:
            me = z * NC + core
            for dz, dc in ZC:
                send(cnt, cnt_all.at[me], 12, s_cnt.at[0], zc(dz, dc)[1])
            keep(cnt, cnt_all.at[me], s_cnt.at[0])
            return
        if part == 2:
            send(cnt_x.at[0], cnt_x.at[1], 13, s_cnt.at[1], owner(1, 0, 0)[2])
            return
        wait(cnt_all, s_cnt.at[0])
        loads = cnt_all[0]
        for e in range(1, NE):
            loads = loads + cnt_all[e]
        cnt_x[0] = loads

    ready = set()

    def mul(g, c0, c1, xl=None):
        arrived = g if xl is None else g + xl
        if arrived not in ready:
            ready.add(arrived)
            wait(gall.at[pl.ds(g * NX, NX if xl is None else 2)], s_gz.at[arrived])
        if g == NY - 1 and xl == 0:
            for c in range(c0, c1):
                wait(ht.at[pl.ds(3 * NX, 2), c], s_hy.at[2, c])
                wait(ht.at[pl.ds(3 * NX + 2, 2), c], s_hy.at[3, c])

        @pl.loop(c0 // 4, c1 // 4)
        def _(pair):
            two = pl.ds(pair * 4, 4)
            at = pl.ds(pl.multiple_of(pair * 4 * step, 4 * step), 4 * step)
            part = None
            for xs in range(NX) if xl is None else (xl, xl + 2):
                q = g * NX + xs
                term = jnp.dot(ht[q, two].reshape(4 * step, half), gall[q].reshape(half, cols), preferred_element_type=jnp.float32)
                part = term if part is None else part + term
            if g == 0:
                acc[at, :] = part
            elif g < NY - 1 or xl == 0:
                acc[at, :] += part
            else:
                out_ref[0, at, :] = (acc[at, :] + part).astype(out_ref.dtype)

    steps = dict(fill=fill, late=late, near=near, count=count, hid=hid, routes=routes, raw=raw, turn=turn, far=far, row=row, relay=relay, pack=pack, mul=mul)
    for name, *which in ORDER:
        steps[name](*which)

    wait(cnt_x.at[1], s_cnt.at[1])
    load_ref[...] = ((cnt_x[0] + cnt_x[1]) / total_pairs)[0, :load_ref.shape[0]]

    sent = (
        meta.at[pl.ds(0, 7)], graw.at[0, 2, 0], graw.at[pl.ds(1, 3), 2], hz.at[:, :, :, pl.ds(0, 7)],
        hz.at[:, :, 0, 0], ht.at[pl.ds(0, 3)], ht.at[pl.ds(0, 2 * NX)], ht.at[pl.ds(0, NX)],
        near_meta.at[pl.ds(0, 4)], graw.at[:, pl.ds(0, 4)], gfar, gnear.at[:, pl.ds(0, 3)],
        cnt_all.at[pl.ds(0, NE - 1)], cnt_x.at[0],
    )
    for i, ref in enumerate(sent):
        wait(ref, s_send.at[i])


def body(hidden, out_grad, route_weight, expert_ids):
    micro, tokens, picks, ff = hidden.shape
    width = out_grad.shape[2]
    experts = lax.axis_size(EP)
    replicas = lax.axis_size(REP)
    cols = width // replicas
    limit = 2 * tokens * picks // experts
    cap = micro * limit
    toks = micro * tokens
    vmem = pl.BlockSpec(memory_space=pltpu.VMEM)
    bf16 = jnp.bfloat16
    dma = pltpu.SemaphoreType.DMA
    grad, load = pl.pallas_call(
        functools.partial(kernel, limit, float(micro * tokens * replicas * picks)),
        out_shape=(
            pltpu.VMEM((1, ff, cols), bf16),
            pltpu.VMEM((experts,), jnp.float32),
        ),
        in_specs=[pl.BlockSpec(memory_space=pl.ANY)] * 4,
        out_specs=(vmem, vmem),
        scratch_shapes=[
            pltpu.VMEM((micro, tokens, picks, ff), bf16),
            pltpu.VMEM((micro, picks, tokens), jnp.int32),
            pltpu.VMEM((micro, picks, tokens), jnp.float32),
            pltpu.VMEM((8, toks), jnp.float32),
            pltpu.VMEM((1, toks * picks), jnp.int32),
            pltpu.VMEM((NY, NEAR, 2, micro, tokens, cols), bf16),
            pltpu.VMEM((2 * NY, 8, toks), jnp.float32),
            pltpu.VMEM((NEAR, NY, 8, toks), jnp.float32),
            pltpu.VMEM((NY, 2 * NC, 2, NEAR, cap, cols), bf16),
            pltpu.VMEM((NY, 2, 3 * NC, 2, cap, cols), bf16),
            pltpu.VMEM((NQ, NC, NZ, cap, cols), bf16),
            pltpu.VMEM((CHUNKS, 2, NE, cap, ff // CHUNKS), bf16),
            pltpu.VMEM((CHUNKS, 2, NC, NZ, cap, ff // CHUNKS), bf16),
            pltpu.VMEM((CHUNKS, 2, ff // CHUNKS, NE * cap), bf16),
            pltpu.VMEM((NQ, CHUNKS, ff // CHUNKS, NE * cap), bf16),
            pltpu.VMEM((ff, cols), jnp.float32),
            pltpu.VMEM((1, toks), jnp.float32),
            pltpu.VMEM((NE, 1, toks), jnp.float32),
            pltpu.VMEM((2, 1, toks), jnp.float32),
            dma((14,)),
            dma((NEAR,)),
            dma((NY,)),
            dma((NY, NEAR)),
            dma((NY + 1,)),
            dma((CHUNKS,)),
            dma((CHUNKS,)),
            dma((4, CHUNKS)),
            dma((2,)),
            dma((3,)),
        ],
        compiler_params=pltpu.CompilerParams(
            collective_id=0, has_side_effects=True, vmem_limit_bytes=62_000_000 // 1024 * 1024
        ),
    )(hidden, expert_ids.transpose(0, 2, 1), route_weight.transpose(0, 2, 1), out_grad)
    return grad, load


def solution(mesh):
    finer = Mesh(mesh.devices.reshape(2, 4, 2, 8, 2), REP_EP)
    placed = (
        P(None, REP_EP, None, None),
        P(None, REP_EP, None),
        P(None, REP_EP, None),
        P(None, REP_EP, None),
    )
    return jax.shard_map(
        body, mesh=finer, in_specs=placed, out_specs=(P(EP, None, REP), P()), check_vma=False
    )
```
